256 devices in a mesh: dp: 8 (over y_hi, x), blk: 32 (over z, y_lo, core).
Axes of the slice: x: 4, y: 4 (y_hi: 2, y_lo: 2; y = y_hi * 2 + y_lo), z: 8, core: 2. Of those that a mesh axis runs over, the one named last changes fastest.
Arguments:
- particles: float32 [4096, 1024], P('blk'), may hold values from -14 to 14
- data_rows: bfloat16 [32768, 1024], P('dp'), may hold values from -0.1875 to 0.1875
- labels: int32 [32768], P('dp'), may hold values from 0 to 1
Outputs:
- descent: float32 [4096, 1024], P('blk')
The draws below stay inside these ranges and needn't reach their ends.
All inputs are finite; a program needn't handle non-finite values.
Results may differ from the reference program's by a relative error of at most 0.0045.
Values may be sent and summed in bfloat16 or wider, within the bound.
A program may use at most 64 MiB of HBM per device.

```python
import math
import jax
import jax.numpy as jnp
from jax import lax

D = 1024
PB = 128
M = 32768
N_BLK = 32


def draw_particles(key, part):
    row_total = PB * N_BLK
    sub_keys = jax.random.split(jax.random.fold_in(key, 4711), 4)
    cluster_total = 64
    centres = jax.random.truncated_normal(sub_keys[0], -4.0, 4.0, (cluster_total, D), jnp.float32)
    member = jax.random.randint(sub_keys[1], (row_total,), 0, cluster_total)
    scales = jnp.exp(jax.random.uniform(sub_keys[2], (cluster_total, 1), jnp.float32, jnp.log(0.5), jnp.log(3.0)))
    jitter = 0.3 * jax.random.truncated_normal(sub_keys[3], -4.0, 4.0, (row_total, D), jnp.float32)
    placed = (scales * centres)[member]
    return (placed + jitter).astype(jnp.float32)


def touch_ends(drawn, rng, low, high):
    spot = [jax.random.randint(jax.random.fold_in(rng, axis), (), 0, length) for axis, length in enumerate(drawn.shape)]
    widest = drawn.shape.index(max(drawn.shape))
    neighbour = spot[:widest] + [(spot[widest] + 1) % drawn.shape[widest]] + spot[widest + 1:]
    return drawn.at[tuple(spot)].set(low).at[tuple(neighbour)].set(high)


def shard_levels(key, dims, shards, smallest, largest):
    gain, own = 1.0, jax.random.fold_in(key, 6)
    for axis_at, parts in shards:
        heights = jnp.exp(jax.random.uniform(jax.random.fold_in(own, axis_at), (parts,), jnp.float32, smallest / len(shards), largest / len(shards)))
        gain = gain * jnp.repeat(heights, dims[axis_at] // parts).reshape([-1 if axis == axis_at else 1 for axis in range(len(dims))])
    return gain


def scatter_about(own_key, extent, scale, limit, cuts=(), dtype=jnp.bfloat16):
    factor_of = shard_levels(own_key, extent, cuts, -0.22, 0.18) if cuts else 1.0
    values = jax.random.normal(own_key, extent, jnp.float32) * scale * factor_of
    return jnp.minimum(jnp.maximum(values, -limit), limit).astype(dtype)


def setup_inputs(seed: int = 0) -> dict:
    key_list = jax.random.split(jax.random.key(seed), 4)
    particles = draw_particles(jax.random.fold_in(key_list[3], 71), 0)
    data_rows = scatter_about(key_list[1], (M, D), D ** -0.5, 0.1875, ((0, 8),))
    labels = touch_ends(jax.random.randint(key_list[2], (M,), 0, 2), jax.random.fold_in(key_list[2], 1), 0, 1).astype(jnp.int32)
    return {"particles": particles, "data_rows": data_rows, "labels": labels}


prior_var = 4.0


def pair_sums(left_x, left_s, right_x, right_s, inv_band):
    feature_count = left_x.shape[1]
    left_xf = left_x.astype(jnp.float32)
    left_sf = left_s.astype(jnp.float32)
    right_xf = right_x.astype(jnp.float32)
    right_sf = right_s.astype(jnp.float32)
    left_norm = jnp.sum(left_xf * left_xf, axis=1)
    right_norm = jnp.sum(right_xf * right_xf, axis=1)
    left_sx = jnp.sum(left_sf * left_xf, axis=1)
    right_sx = jnp.sum(right_sf * right_xf, axis=1)
    gram_xx = jnp.einsum("id,jd->ij", left_x, right_x, preferred_element_type=jnp.float32)
    gram_ss = jnp.einsum("id,jd->ij", left_s, right_s, preferred_element_type=jnp.float32)
    cross_dot = jnp.einsum("id,jd->ij", jnp.concatenate([left_x, left_s], axis=1),
                           jnp.concatenate([right_s, right_x], axis=1), preferred_element_type=jnp.float32)
    distance = left_norm[:, None] + right_norm[None, :] - 2.0 * gram_xx
    kernel = jnp.exp(-0.5 * inv_band * distance)
    bracket = (gram_ss + inv_band * (left_sx[:, None] - cross_dot + right_sx[None, :])
               + feature_count * inv_band - inv_band * inv_band * distance)
    weighted_kernel = kernel * bracket
    kernel_sum = jnp.sum(kernel, axis=1)
    weighted_sum = jnp.sum(weighted_kernel, axis=1)
    both_rows = jnp.dot(kernel.astype(jnp.bfloat16), jnp.concatenate([right_x, right_s], axis=1),
                        preferred_element_type=jnp.float32)
    kernel_x = both_rows[:, :feature_count]
    kernel_s = both_rows[:, feature_count:]
    weighted_x = jnp.dot(weighted_kernel.astype(jnp.bfloat16), right_x, preferred_element_type=jnp.float32)
    return (kernel_sum, weighted_sum, kernel_x, kernel_s, weighted_x)


def forces(left_x, left_s, sums, inv_band, particle_count):
    kernel_sum, weighted_sum, kernel_x, kernel_s, weighted_x = sums
    left_xf = left_x.astype(jnp.float32)
    left_sf = left_s.astype(jnp.float32)
    spread = kernel_sum[:, None] * left_xf - kernel_x
    score_force = (kernel_s + inv_band * spread) / particle_count
    place_force = (-inv_band * (weighted_sum[:, None] * left_xf - weighted_x)
                   + inv_band * (kernel_sum[:, None] * left_sf - kernel_s)
                   - 2.0 * inv_band * inv_band * spread) / particle_count
    return score_force, place_force


def reference(particles, data_rows, labels):
    particle_count, feature_count = particles.shape
    inv_band = 1.0 / feature_count
    block_rows = math.gcd(particle_count, 512)
    block_count = particle_count // block_rows
    label_vals = labels.astype(jnp.float32)
    x_low = particles.astype(jnp.bfloat16)
    stacked_x = x_low.reshape(block_count, block_rows, feature_count)
    stacked_p = particles.reshape(block_count, block_rows, feature_count)

    def score_block(pieces):
        x_block, p_block = pieces
        logits = jnp.einsum("pd,md->pm", x_block, data_rows, preferred_element_type=jnp.float32)
        probability = jax.nn.sigmoid(logits)
        residual = (label_vals[None, :] - probability).astype(jnp.bfloat16)
        return jnp.dot(residual, data_rows, preferred_element_type=jnp.float32) - p_block / prior_var

    scores = lax.map(score_block, (stacked_x, stacked_p)).reshape(particle_count, feature_count)
    s_low = scores.astype(jnp.bfloat16)
    stacked_s = s_low.reshape(block_count, block_rows, feature_count)

    def descent_block(pieces):
        x_block, s_block = pieces
        sums = pair_sums(x_block, s_block, x_low, s_low, inv_band)
        score_force, place_force = forces(x_block, s_block, sums, inv_band, particle_count)
        logits = jnp.einsum("pd,md->pm", x_block, data_rows, preferred_element_type=jnp.float32)
        probability = jax.nn.sigmoid(logits)
        curvature = probability * (1.0 - probability)
        projected = jnp.einsum("pd,md->pm", score_force.astype(jnp.bfloat16), data_rows,
                               preferred_element_type=jnp.float32)
        weighted_rows = (curvature * projected).astype(jnp.bfloat16)
        data_term = jnp.dot(weighted_rows, data_rows, preferred_element_type=jnp.float32)
        return data_term - place_force + score_force / prior_var

    return lax.map(descent_block, (stacked_x, stacked_s)).reshape(particle_count, feature_count)
```

```python
import jax
import jax.numpy as jnp
from jax import lax
from jax.experimental import pallas as pl
from jax.experimental.pallas import tpu as pltpu
from jax.sharding import Mesh
from jax.sharding import PartitionSpec as P

DP = ("yh", "x")
BLK = ("z", "yl", "c")
prior_var = 4.0
NCH = 2
F32 = jnp.float32
BF16 = jnp.bfloat16

PEERS = ((1, 2), (1, 1), (1, 3), (0, 2), (1, 0), (0, 1), (0, 3))


def dot_t(a, b):
    return lax.dot_general(a, b, (((1,), (1,)), ((), ())), preferred_element_type=F32)


def dot_n(a, b):
    return lax.dot_general(a, b, (((1,), (0,)), ((), ())), preferred_element_type=F32)


def as_row(col, rows):
    return jnp.broadcast_to(col, (col.shape[0], rows)).T


def make_kernel(feature_count, data_count, particle_count):
    D = feature_count
    inv_band = 1.0 / D
    SR = 16
    NS = 8
    PB = SR * NS
    NZ = 8
    CW = D // NCH
    DCH = 8
    DR = data_count // DCH

    def kernel(
        part_hbm, data_hbm, lab_hbm, out_ref,
        data, part, lab, xl, resid, curv, psb, rbuf, left_s, glow, rx, rs,
        kf, dist, kb, wb, place, own_force, fin,
        load_sem, dps, dpr, bsx, bax, bbx, bcx, bdx, bss, bas, bbs, bcs, bds,
    ):
        yh, x = lax.axis_index("yh"), lax.axis_index("x")
        z, yl, c = lax.axis_index("z"), lax.axis_index("yl"), lax.axis_index("c")
        g = yh * 4 + x
        y = yh * 2 + yl
        ny = lax.rem(y + 1 + 2 * c, 4)
        py = lax.rem(y + 3 + 2 * c, 4)

        def at_dp(dy, dx):
            return lax.rem(yh + dy, 2), lax.rem(x + dx, 4)

        def dev_dp(dy, dx):
            ty, tx = at_dp(dy, dx)
            return {"yh": ty, "x": tx}

        def dev_z(d):
            return {"z": lax.rem(z + d, NZ)}

        def dev_y(t):
            return {"yh": t // 2, "yl": lax.rem(t, 2)}

        dev_core = {"c": 1 - c}
        everyone = (
            [dev_dp(*p) for p in PEERS] + [dev_z(d) for d in range(1, NZ)]
            + [dev_y(ny), dev_y(py), dev_core]
        )
        barrier = pltpu.get_barrier_semaphore()
        for dev in everyone:
            pl.semaphore_signal(barrier, inc=1, device_id=dev, device_id_type=pl.DeviceIdType.MESH)

        load_part = pltpu.make_async_copy(part_hbm, part, load_sem.at[DCH])
        load_lab = pltpu.make_async_copy(lab_hbm, lab, load_sem.at[DCH + 1])
        load_part.start()
        load_lab.start()

        def load_data(i):
            rows = pl.ds(pl.multiple_of(i * DR, DR), DR)
            return pltpu.make_async_copy(data_hbm.at[rows], data.at[rows], load_sem.at[i])

        for i in range(DCH):
            load_data(i).start()

        def remote(src, dst, ssem, rsem, dev):
            return pltpu.make_async_remote_copy(
                src_ref=src, dst_ref=dst, send_sem=ssem, recv_sem=rsem,
                device_id=dev, device_id_type=pl.DeviceIdType.MESH,
            )

        def cols(ch):
            return pl.ds(ch * CW, CW)

        def rs_send(phase, ch):
            for dy, dx in PEERS:
                ty, tx = at_dp(dy, dx)
                remote(
                    psb.at[phase, ty * 4 + tx, :, cols(ch)],
                    rbuf.at[phase, dy * 4 + dx, :, cols(ch)],
                    dps.at[phase, 0, ch], dpr.at[phase, 0, ch], {"yh": ty, "x": tx},
                ).start()

        def seven(phase, kind, ch):
            ref = rbuf.at[phase, pl.ds(1, NS - 1), :, cols(ch)]
            return remote(ref, ref, dps.at[phase, kind, ch], dpr.at[phase, kind, ch], dev_core)

        def rs_total(phase, ch):
            seven(phase, 0, ch).wait_recv()
            total = psb[phase, g, :, cols(ch)].astype(F32)
            for d in range(1, NS):
                total = total + rbuf[phase, d, :, cols(ch)].astype(F32)
            return total

        def ag_send(phase, ref, ch):
            for dy, dx in PEERS:
                remote(
                    ref.at[g, :, cols(ch)], ref.at[g, :, cols(ch)],
                    dps.at[phase, 1, ch], dpr.at[phase, 1, ch], dev_dp(dy, dx),
                ).start()

        def ag_wait(phase, ch):
            seven(phase, 1, ch).wait_recv()

        class Gather:
            def __init__(self, buf, send, a, b, cc, d):
                self.buf, self.send, self.a, self.b, self.c, self.d = buf, send, a, b, cc, d

            def start(self):
                for d in (4, 3, 5, 2, 6, 1, 7):
                    remote(self.buf.at[0], self.buf.at[d], self.send, self.a.at[d], dev_z(d)).start()
                self.pass_on(0)

            def pass_on(self, d):
                remote(self.buf.at[d], self.buf.at[8 + d], self.send, self.b.at[d], dev_y(ny)).start()
                remote(self.buf.at[d], self.buf.at[16 + d], self.send, self.c, dev_core).start()

            def forward_a(self, d):
                remote(self.buf.at[d], self.buf.at[d], self.send, self.a.at[d], dev_core).wait_recv()
                self.pass_on(d)

            def forward_b(self, d):
                remote(self.buf.at[d], self.buf.at[8 + d], self.send, self.b.at[d], dev_core).wait_recv()
                remote(self.buf.at[8 + d], self.buf.at[24 + d], self.send, self.d, dev_core).start()

            def wait_c(self):
                ref = self.buf.at[pl.ds(16, 8)]
                remote(ref, ref, self.send, self.c, dev_core).wait_recv()

            def wait_d(self):
                ref = self.buf.at[pl.ds(24, 8)]
                remote(ref, ref, self.send, self.d, dev_core).wait_recv()

            def drain(self):
                ref = self.buf.at[pl.ds(0, 31)]
                remote(ref, ref, self.send, self.d, dev_core).wait_send()

        ORDER = (1, 7, 2, 6, 3, 5, 4)
        gx = Gather(rx, bsx, bax, bbx, bcx, bdx)
        gs = Gather(rs, bss, bas, bbs, bcs, bds)

        load_part.wait()
        xl[...] = part[...].astype(BF16)
        rx[0] = xl[g]
        load_lab.wait()

        def logits_step(i):
            load_data(i).wait()
            rows = pl.ds(pl.multiple_of(i * DR, DR), DR)
            logits = dot_t(xl[...].reshape(PB, D), data[rows, :])
            p = jax.nn.sigmoid(logits)
            resid[:, rows] = (lab[:, rows].astype(F32) - p).astype(BF16)
            curv[:, rows] = p * (1.0 - p)

        pl.semaphore_wait(barrier, len(everyone))
        gx.start()

        @pl.loop(0, DCH)
        def _(i):
            logits_step(i)

        for ch in range(NCH):
            part_score = dot_n(resid[...], data[:, cols(ch)])
            psb[0, :, :, cols(ch)] = part_score.astype(BF16).reshape(NS, SR, CW)
            rs_send(0, ch)

        for d in ORDER:
            gx.forward_a(d)

        for ch in range(NCH):
            score = rs_total(0, ch) - part[g, :, cols(ch)] / prior_var
            own = score.astype(BF16)
            rs[0, :, cols(ch)] = own
            left_s[g, :, cols(ch)] = own
            ag_send(0, left_s, ch)
        gs.start()

        for d in (0,) + ORDER:
            gx.forward_b(d)
        gx.wait_c()
        gx.wait_d()

        xlow = xl[...].reshape(PB, D)
        xf = xlow.astype(F32)
        left_norm = jnp.sum(xf * xf, axis=1, keepdims=True)
        right_x = rx[...].reshape(32 * SR, D)
        rxf = right_x.astype(F32)
        right_norm = jnp.sum(rxf * rxf, axis=1, keepdims=True)
        distance = left_norm + as_row(right_norm, PB) - 2.0 * dot_t(xlow, right_x)
        kernel_val = jnp.exp(-0.5 * inv_band * distance)
        kf[...] = kernel_val
        dist[...] = distance
        kb[...] = kernel_val.astype(BF16)
        kernel_sum = jnp.sum(kernel_val, axis=1, keepdims=True)

        for d in ORDER:
            gs.forward_a(d)
        for ch in range(NCH):
            ag_wait(0, ch)
        for d in (0,) + ORDER:
            gs.forward_b(d)
        gs.wait_c()
        gs.wait_d()

        slow = left_s[...].reshape(PB, D)
        left_sx = jnp.sum(slow.astype(F32) * xf, axis=1, keepdims=True)
        right_s = rs[...].reshape(32 * SR, D)
        right_sx = jnp.sum(right_s.astype(F32) * rxf, axis=1, keepdims=True)
        gram_ss = dot_t(slow, right_s)
        cross = dot_t(xlow, right_s) + dot_t(slow, right_x)
        bracket = (
            gram_ss + inv_band * (left_sx - cross + as_row(right_sx, PB))
            + D * inv_band - inv_band * inv_band * dist[...]
        )
        weighted = kf[...] * bracket
        wb[...] = weighted.astype(BF16)
        weighted_sum = jnp.sum(weighted, axis=1, keepdims=True)

        for ch in range(NCH):
            rxc = rx[:, :, cols(ch)].reshape(32 * SR, CW)
            rsc = rs[:, :, cols(ch)].reshape(32 * SR, CW)
            kernel_x = dot_n(kb[...], rxc)
            kernel_s = dot_n(kb[...], rsc)
            weighted_x = dot_n(wb[...], rxc)
            xc = xl[:, :, cols(ch)].reshape(PB, CW).astype(F32)
            sc = left_s[:, :, cols(ch)].reshape(PB, CW).astype(F32)
            spread = kernel_sum * xc - kernel_x
            force = (kernel_s + inv_band * spread) / particle_count
            psb[1, :, :, cols(ch)] = force.astype(BF16).reshape(NS, SR, CW)
            rs_send(1, ch)
            place[:, cols(ch)] = (
                -inv_band * (weighted_sum * xc - weighted_x)
                + inv_band * (kernel_sum * sc - kernel_s)
                - 2.0 * inv_band * inv_band * spread
            ) / particle_count

        for ch in range(NCH):
            total = rs_total(1, ch)
            own_force[:, cols(ch)] = total
            glow[g, :, cols(ch)] = total.astype(BF16)
            ag_send(1, glow, ch)
        for ch in range(NCH):
            ag_wait(1, ch)

        @pl.loop(0, DCH)
        def _(i):
            rows = pl.ds(pl.multiple_of(i * DR, DR), DR)
            projected = dot_t(glow[...].reshape(PB, D), data[rows, :])
            resid[:, rows] = (curv[:, rows] * projected).astype(BF16)

        for ch in range(NCH):
            term = dot_n(resid[...], data[:, cols(ch)]) - place[:, cols(ch)]
            psb[2, :, :, cols(ch)] = term.astype(BF16).reshape(NS, SR, CW)
            rs_send(2, ch)

        for ch in range(NCH):
            total = rs_total(2, ch) + own_force[:, cols(ch)] / prior_var
            fin[g, :, cols(ch)] = total.astype(BF16)
            ag_send(2, fin, ch)
        for ch in range(NCH):
            ag_wait(2, ch)
            out_ref[:, cols(ch)] = fin[:, :, cols(ch)].reshape(PB, CW).astype(F32)

        gx.drain()
        gs.drain()
        for phase in range(3):
            for kind in range(2):
                for ch in range(NCH):
                    seven(phase, kind, ch).wait_send()

    V = pltpu.VMEM
    S = pltpu.SemaphoreType.DMA
    scratch = [
        V((data_count, D), BF16), V((NS, SR, D), F32), V((1, data_count), jnp.int32),
        V((NS, SR, D), BF16), V((PB, data_count), BF16), V((PB, data_count), F32),
        V((3, NS, SR, D), BF16), V((3, NS, SR, D), BF16), V((NS, SR, D), BF16), V((NS, SR, D), BF16),
        V((32, SR, D), BF16), V((32, SR, D), BF16),
        V((PB, 32 * SR), F32), V((PB, 32 * SR), F32), V((PB, 32 * SR), BF16), V((PB, 32 * SR), BF16),
        V((PB, D), F32), V((SR, D), F32), V((NS, SR, D), BF16),
        S((DCH + 2,)), S((3, 2, NCH)), S((3, 2, NCH)),
        S, S((NZ,)), S((NZ,)), S, S,
        S, S((NZ,)), S((NZ,)), S, S,
    ]
    return kernel, scratch


def solution(mesh):
    torus = Mesh(mesh.devices.reshape(2, 4, 8, 2, 2), DP + BLK)

    def shards(particles, data_rows, labels):
        rows, feature_count = particles.shape
        kernel, scratch = make_kernel(feature_count, data_rows.shape[0], rows * 32)
        return pl.pallas_call(
            kernel,
            out_shape=jax.ShapeDtypeStruct((rows, feature_count), F32),
            in_specs=[pl.BlockSpec(memory_space=pl.ANY)] * 3,
            out_specs=pl.BlockSpec(memory_space=pltpu.VMEM),
            scratch_shapes=scratch,
            compiler_params=pltpu.CompilerParams(
                collective_id=0, has_side_effects=True, vmem_limit_bytes=60 * 1024 * 1024
            ),
        )(particles.reshape(8, 16, feature_count), data_rows, labels.reshape(1, -1))

    return jax.shard_map(
        shards,
        mesh=torus,
        in_specs=(P(BLK, None), P(DP, None), P(DP)),
        out_specs=P(BLK, None),
        check_vma=False,
    )
```

```python
import jax
import jax.numpy as jnp
from jax import lax
from jax.experimental import pallas as pl
from jax.experimental.pallas import tpu as pltpu
from jax.sharding import Mesh
from jax.sharding import PartitionSpec as P

DP = ("yh", "x")
BLK = ("z", "yl", "c")
prior_var = 4.0
NCH = 2
F32 = jnp.float32
BF16 = jnp.bfloat16

PEERS = ((1, 2), (1, 1), (1, 3), (0, 2), (1, 0), (0, 1), (0, 3))


def dot_t(a, b):
    return lax.dot_general(a, b, (((1,), (1,)), ((), ())), preferred_element_type=F32)


def dot_n(a, b):
    return lax.dot_general(a, b, (((1,), (0,)), ((), ())), preferred_element_type=F32)


def as_row(col, rows):
    return jnp.broadcast_to(col, (col.shape[0], rows)).T


def make_kernel(feature_count, data_count, particle_count):
    D = feature_count
    inv_band = 1.0 / D
    SR = 16
    NS = 8
    PB = SR * NS
    NZ = 8
    CW = D // NCH
    DCH = 8
    DR = data_count // DCH

    def kernel(
        part_hbm, data_hbm, lab_hbm, out_ref,
        data, part, lab, xl, resid, curv, psb, rbuf, left_s, glow, rx, rs,
        kf, dist, kb, wb, place, own_force, data_t, lg, acc, ks, spread, ksum,
        load_sem, dps, dpr, bsx, bax, bbx, bcx, bdx, bss, bas, bbs, bcs, bds,
    ):
        yh, x = lax.axis_index("yh"), lax.axis_index("x")
        z, yl, c = lax.axis_index("z"), lax.axis_index("yl"), lax.axis_index("c")
        g = yh * 4 + x
        y = yh * 2 + yl
        ny = lax.rem(y + 1 + 2 * c, 4)
        py = lax.rem(y + 3 + 2 * c, 4)

        def at_dp(dy, dx):
            return lax.rem(yh + dy, 2), lax.rem(x + dx, 4)

        def dev_dp(dy, dx):
            ty, tx = at_dp(dy, dx)
            return {"yh": ty, "x": tx}

        def dev_z(d):
            return {"z": lax.rem(z + d, NZ)}

        def dev_y(t):
            return {"yh": t // 2, "yl": lax.rem(t, 2)}

        dev_core = {"c": 1 - c}
        everyone = (
            [dev_dp(*p) for p in PEERS] + [dev_z(d) for d in range(1, NZ)]
            + [dev_y(ny), dev_y(py), dev_core]
        )
        barrier = pltpu.get_barrier_semaphore()
        for dev in everyone:
            pl.semaphore_signal(barrier, inc=1, device_id=dev, device_id_type=pl.DeviceIdType.MESH)

        load_part = pltpu.make_async_copy(part_hbm, part, load_sem.at[DCH])
        load_lab = pltpu.make_async_copy(lab_hbm, lab, load_sem.at[DCH + 1])
        load_part.start()
        load_lab.start()

        def load_data(i):
            rows = pl.ds(pl.multiple_of(i * DR, DR), DR)
            return pltpu.make_async_copy(data_hbm.at[rows], data.at[rows], load_sem.at[i])

        for i in range(DCH):
            load_data(i).start()

        def remote(src, dst, ssem, rsem, dev):
            return pltpu.make_async_remote_copy(
                src_ref=src, dst_ref=dst, send_sem=ssem, recv_sem=rsem,
                device_id=dev, device_id_type=pl.DeviceIdType.MESH,
            )

        def cols(ch):
            return pl.ds(ch * CW, CW)

        def rs_send(phase, ch):
            for dy, dx in PEERS:
                ty, tx = at_dp(dy, dx)
                remote(
                    psb.at[phase, ty * 4 + tx, :, cols(ch)],
                    rbuf.at[phase, dy * 4 + dx, :, cols(ch)],
                    dps.at[phase, 0, ch], dpr.at[phase, 0, ch], {"yh": ty, "x": tx},
                ).start()

        def seven(phase, kind, ch):
            ref = rbuf.at[phase, pl.ds(1, NS - 1), :, cols(ch)]
            return remote(ref, ref, dps.at[phase, kind, ch], dpr.at[phase, kind, ch], dev_core)

        def rs_total(phase, ch):
            seven(phase, 0, ch).wait_recv()
            total = psb[phase, g, :, cols(ch)].astype(F32)
            for d in range(1, NS):
                total = total + rbuf[phase, d, :, cols(ch)].astype(F32)
            return total

        def ag_send(phase, ref, ch):
            for dy, dx in PEERS:
                remote(
                    ref.at[g, :, cols(ch)], ref.at[g, :, cols(ch)],
                    dps.at[phase, 1, ch], dpr.at[phase, 1, ch], dev_dp(dy, dx),
                ).start()

        def ag_wait(phase, ch):
            seven(phase, 1, ch).wait_recv()

        ORDER = (4, 3, 5, 2, 6, 1, 7)

        class Gather:
            def __init__(self, buf, send, a, b, cc, d):
                self.buf, self.send, self.a, self.b, self.c, self.d = buf, send, a, b, cc, d

            def start(self):
                for d in ORDER:
                    remote(self.buf.at[0], self.buf.at[d], self.send, self.a.at[d], dev_z(d)).start()
                self.pass_on(0)

            def pass_on(self, d):
                remote(self.buf.at[d], self.buf.at[16 + d], self.send, self.b.at[d], dev_y(ny)).start()
                remote(self.buf.at[d], self.buf.at[8 + d], self.send, self.c, dev_core).start()

            def forward_a(self, d):
                remote(self.buf.at[d], self.buf.at[d], self.send, self.a.at[d], dev_core).wait_recv()
                self.pass_on(d)

            def forward_b(self, d):
                remote(self.buf.at[d], self.buf.at[16 + d], self.send, self.b.at[d], dev_core).wait_recv()
                remote(self.buf.at[16 + d], self.buf.at[24 + d], self.send, self.d, dev_core).start()

            def wait_c(self):
                ref = self.buf.at[pl.ds(8, 8)]
                remote(ref, ref, self.send, self.c, dev_core).wait_recv()

            def wait_d(self):
                ref = self.buf.at[pl.ds(24, 8)]
                remote(ref, ref, self.send, self.d, dev_core).wait_recv()

            def drain(self):
                ref = self.buf.at[pl.ds(0, 31)]
                remote(ref, ref, self.send, self.d, dev_core).wait_send()

        gx = Gather(rx, bsx, bax, bbx, bcx, bdx)
        gs = Gather(rs, bss, bas, bbs, bcs, bds)

        with jax.named_scope("load_x"):
            load_part.wait()
            xl[...] = part[...].astype(BF16)
            rx[0] = xl[g]
            load_lab.wait()

        with jax.named_scope("barrier"):
            pl.semaphore_wait(barrier, len(everyone))
            gx.start()

        def rows_of(i):
            return pl.ds(i * DR, DR)

        def turn(i):
            load_data(i).wait()
            data_t[:, rows_of(i)] = data[rows_of(i), :].T

        def logits(i):
            lg[i % 2] = dot_n(xl[...].reshape(PB, D), data_t[:, rows_of(i)])

        def squash(i):
            p = jax.nn.sigmoid(lg[i % 2])
            resid[:, rows_of(i)] = (lab[:, rows_of(i)].astype(F32) - p).astype(BF16)
            curv[:, rows_of(i)] = p * (1.0 - p)

        def collect(i):
            term = dot_n(resid[:, rows_of(i)], data[rows_of(i), :])
            if i == 0:
                acc[...] = term
            elif i < DCH - 1:
                acc[...] += term
            else:
                psb[0] = (acc[...] + term).astype(BF16).reshape(NS, SR, D)

        with jax.named_scope("score"):
            stages = (turn, logits, squash, collect)
            for step in range(DCH + len(stages) - 1):
                for k, stage in enumerate(stages):
                    if 0 <= step - k < DCH:
                        stage(step - k)
            for ch in range(NCH):
                rs_send(0, ch)

        with jax.named_scope("fwd_a_x"):
            for d in ORDER:
                gx.forward_a(d)

        with jax.named_scope("rs0"):
            for ch in range(NCH):
                score = rs_total(0, ch) - part[g, :, cols(ch)] / prior_var
                own = score.astype(BF16)
                rs[0, :, cols(ch)] = own
                left_s[g, :, cols(ch)] = own
            gs.start()
            for ch in range(NCH):
                ag_send(0, left_s, ch)

        with jax.named_scope("fwd_b_x"):
            for d in (0,) + ORDER:
                gx.forward_b(d)
            gx.wait_c()
            gx.wait_d()

        with jax.named_scope("pair_x"):
            xlow = xl[...].reshape(PB, D)
            xf = xlow.astype(F32)
            left_norm = jnp.sum(xf * xf, axis=1, keepdims=True)
            right_x = rx[...].reshape(32 * SR, D)
            rxf = right_x.astype(F32)
            right_norm = jnp.sum(rxf * rxf, axis=1, keepdims=True)
            distance = left_norm + as_row(right_norm, PB) - 2.0 * dot_t(xlow, right_x)
            kernel_val = jnp.exp(-0.5 * inv_band * distance)
            kf[...] = kernel_val
            dist[...] = distance
            kb[...] = kernel_val.astype(BF16)
            kernel_sum = jnp.sum(kernel_val, axis=1, keepdims=True)
            ksum[...] = kernel_sum
            spread[...] = kernel_sum * xf - dot_n(kb[...], right_x)

        with jax.named_scope("fwd_a_s"):
            for d in ORDER:
                gs.forward_a(d)
            gs.wait_c()
        with jax.named_scope("fwd_b_s"):
            for d in (0,) + ORDER:
                gs.forward_b(d)
            gs.wait_d()

        with jax.named_scope("force"):
            for ch in range(NCH):
                kernel_s = dot_n(kb[...], rs[:, :, cols(ch)].reshape(32 * SR, CW))
                ks[:, cols(ch)] = kernel_s
                force = (kernel_s + inv_band * spread[:, cols(ch)]) / particle_count
                psb[1, :, :, cols(ch)] = force.astype(BF16).reshape(NS, SR, CW)
                rs_send(1, ch)

        with jax.named_scope("place"):
            for ch in range(NCH):
                ag_wait(0, ch)
            slow = left_s[...].reshape(PB, D)
            xlow = xl[...].reshape(PB, D)
            xf = xlow.astype(F32)
            sf = slow.astype(F32)
            left_sx = jnp.sum(sf * xf, axis=1, keepdims=True)
            right_x = rx[...].reshape(32 * SR, D)
            right_s = rs[...].reshape(32 * SR, D)
            right_sx = jnp.sum(right_s.astype(F32) * right_x.astype(F32), axis=1, keepdims=True)
            cross = dot_t(xlow, right_s) + dot_t(slow, right_x)
            bracket = (
                dot_t(slow, right_s) + inv_band * (left_sx - cross + as_row(right_sx, PB))
                + D * inv_band - inv_band * inv_band * dist[...]
            )
            weighted = kf[...] * bracket
            wb[...] = weighted.astype(BF16)
            weighted_sum = jnp.sum(weighted, axis=1, keepdims=True)
            weighted_x = dot_n(wb[...], right_x)
            place[...] = (
                -inv_band * (weighted_sum * xf - weighted_x)
                + inv_band * (ksum[...] * sf - ks[...])
                - 2.0 * inv_band * inv_band * spread[...]
            ) / particle_count

        with jax.named_scope("rs1"):
            for ch in range(NCH):
                total = rs_total(1, ch)
                own_force[:, cols(ch)] = total
                glow[g, :, cols(ch)] = total.astype(BF16)
                ag_send(1, glow, ch)
        with jax.named_scope("ag1"):
            for ch in range(NCH):
                ag_wait(1, ch)

        with jax.named_scope("proj"):
            for i in range(DCH):
                projected = dot_n(glow[...].reshape(PB, D), data_t[:, rows_of(i)])
                resid[:, rows_of(i)] = (curv[:, rows_of(i)] * projected).astype(BF16)

        with jax.named_scope("term"):
            for ch in range(NCH):
                term = dot_n(resid[...], data[:, cols(ch)]) - place[:, cols(ch)]
                psb[2, :, :, cols(ch)] = term.astype(BF16).reshape(NS, SR, CW)
                rs_send(2, ch)

        with jax.named_scope("rs2"):
            for ch in range(NCH):
                total = rs_total(2, ch) + own_force[:, cols(ch)] / prior_var
                out_ref[g, :, cols(ch)] = total.astype(BF16)
                ag_send(2, out_ref, ch)
        with jax.named_scope("ag2"):
            for ch in range(NCH):
                ag_wait(2, ch)

        gx.drain()
        gs.drain()
        for phase in range(3):
            for kind in range(2):
                for ch in range(NCH):
                    seven(phase, kind, ch).wait_send()

    V = pltpu.VMEM
    S = pltpu.SemaphoreType.DMA
    scratch = [
        V((data_count, D), BF16), V((NS, SR, D), F32), V((1, data_count), jnp.int32),
        V((NS, SR, D), BF16), V((PB, data_count), BF16), V((PB, data_count), F32),
        V((3, NS, SR, D), BF16), V((3, NS, SR, D), BF16), V((NS, SR, D), BF16), V((NS, SR, D), BF16),
        V((32, SR, D), BF16), V((32, SR, D), BF16),
        V((PB, 32 * SR), F32), V((PB, 32 * SR), F32), V((PB, 32 * SR), BF16), V((PB, 32 * SR), BF16),
        V((PB, D), F32), V((SR, D), F32),
        V((D, data_count), BF16), V((2, PB, DR), F32), V((PB, D), F32), V((PB, D), F32), V((PB, D), F32),
        V((PB, 1), F32),
        S((DCH + 2,)), S((3, 2, NCH)), S((3, 2, NCH)),
        S, S((NZ,)), S((NZ,)), S, S,
        S, S((NZ,)), S((NZ,)), S, S,
    ]
    return kernel, scratch


def solution(mesh):
    torus = Mesh(mesh.devices.reshape(2, 4, 8, 2, 2), DP + BLK)

    def shards(particles, data_rows, labels):
        rows, feature_count = particles.shape
        kernel, scratch = make_kernel(feature_count, data_rows.shape[0], rows * 32)
        descent = pl.pallas_call(
            kernel,
            out_shape=jax.ShapeDtypeStruct((8, 16, feature_count), BF16),
            in_specs=[pl.BlockSpec(memory_space=pl.ANY)] * 3,
            out_specs=pl.BlockSpec(memory_space=pltpu.VMEM),
            scratch_shapes=scratch,
            compiler_params=pltpu.CompilerParams(
                collective_id=0, has_side_effects=True, vmem_limit_bytes=44 * 1024 * 1024
            ),
        )(*[pltpu.with_memory_space_constraint(v, pltpu.HBM) for v in (particles.reshape(8, 16, feature_count), data_rows, labels.reshape(1, -1))])
        return descent.reshape(rows, feature_count).astype(F32)

    return jax.shard_map(
        shards,
        mesh=torus,
        in_specs=(P(BLK, None), P(DP, None), P(DP)),
        out_specs=P(BLK, None),
        check_vma=False,
    )
```

```python
import jax
import jax.numpy as jnp
from jax import lax
from jax.experimental import pallas as pl
from jax.experimental.pallas import tpu as pltpu
from jax.sharding import Mesh
from jax.sharding import PartitionSpec as P

DP = ("yh", "x")
BLK = ("z", "yl", "c")
prior_var = 4.0
NCH = 2
F32 = jnp.float32
BF16 = jnp.bfloat16

PEERS = ((1, 2), (1, 1), (1, 3), (0, 2), (1, 0), (0, 1), (0, 3))

OTHERS = ((0, 2), (1, 2), (0, 1), (1, 1), (0, 3), (1, 3), (1, 0), (0, 0))
FORCE_TO = (
    (1, 1, 2), (0, 0, 2), (0, 1, 2), (1, 1, 1), (1, 1, 3), (0, 0, 1), (0, 1, 1), (0, 0, 3),
    (0, 1, 3), (1, 0, 2), (1, 1, 0), (0, 1, 0), (0, 0, 0), (1, 0, 1), (1, 0, 3),
)
ORDER = (4, 3, 5, 2, 6, 1, 7)
FIRST = 3


def dot_t(a, b):
    return lax.dot_general(a, b, (((1,), (1,)), ((), ())), preferred_element_type=F32)


def dot_n(a, b):
    return lax.dot_general(a, b, (((1,), (0,)), ((), ())), preferred_element_type=F32)


def as_row(col, rows):
    return jnp.broadcast_to(col, (col.shape[0], rows)).T


def make_kernel(feature_count, data_count, particle_count):
    D = feature_count
    inv_band = 1.0 / D
    SR = 16
    NS = 8
    PB = SR * NS
    NZ = 8
    NR = 2 * NZ * SR
    CW = D // NCH
    DCH = 8
    DR = data_count // DCH

    def kernel(
        part_hbm, data_hbm, lab_hbm, out_ref,
        data, part, lab, lx, ls, resid, curv, psb, psf, psp, rbuf, rforce, rplace, glow, rx, rs,
        kf, dist, kb, wb, place, own_force, data_t, lg, acc, ks, spread, ksum,
        load_sem, sent, rsr, agr, gxr, gsr, nbr,
    ):
        yh, x = lax.axis_index("yh"), lax.axis_index("x")
        z, yl, c = lax.axis_index("z"), lax.axis_index("yl"), lax.axis_index("c")
        g = yh * 4 + x
        y = yh * 2 + yl

        def at_dp(dy, dx):
            return lax.rem(yh + dy, 2), lax.rem(x + dx, 4)

        def dev_dp(dy, dx):
            ty, tx = at_dp(dy, dx)
            return {"yh": ty, "x": tx}

        def dev_other(dy, dx):
            return {**dev_dp(dy, dx), "yl": 1 - yl}

        def dev_z(d):
            return {"z": lax.rem(z + d, NZ)}

        def dev_y(t):
            return {"yh": t // 2, "yl": lax.rem(t, 2)}

        y_up, y_down = dev_y(lax.rem(y + 1, 4)), dev_y(lax.rem(y + 3, 4))
        dev_core = {"c": 1 - c}
        everyone = (
            [dev_dp(*p) for p in PEERS] + [dev_other(*p) for p in OTHERS]
            + [dev_z(d) for d in range(1, NZ)] + [dev_core]
        )
        barrier = pltpu.get_barrier_semaphore()
        for dev in everyone:
            pl.semaphore_signal(barrier, inc=1, device_id=dev, device_id_type=pl.DeviceIdType.MESH)

        load_part = pltpu.make_async_copy(part_hbm, part, load_sem.at[DCH])
        load_lab = pltpu.make_async_copy(lab_hbm, lab, load_sem.at[DCH + 1])
        load_part.start()
        load_lab.start()

        def rows_of(i):
            return pl.ds(i * DR, DR)

        def load_data(i):
            return pltpu.make_async_copy(data_hbm.at[rows_of(i)], data.at[rows_of(i)], load_sem.at[i])

        for i in range(DCH):
            load_data(i).start()

        def remote(src, dst, ssem, rsem, dev):
            return pltpu.make_async_remote_copy(
                src_ref=src, dst_ref=dst, send_sem=ssem, recv_sem=rsem,
                device_id=dev, device_id_type=pl.DeviceIdType.MESH,
            )

        def cols(ch):
            return pl.ds(ch * CW, CW)

        def wait_bytes(shares, rsem, width):
            ref = rforce.at[pl.ds(0, shares), :, width]
            remote(ref, ref, sent.at[0], rsem, dev_core).wait_recv()

        def rs_send(k, src, dst, ch):
            for dy, dx in PEERS:
                ty, tx = at_dp(dy, dx)
                remote(
                    src.at[ty * 4 + tx, :, cols(ch)], dst.at[dy * 4 + dx, :, cols(ch)],
                    sent.at[k], rsr.at[k, ch], {"yh": ty, "x": tx},
                ).start()

        def rs_total(k, src, buf, ch, sources):
            wait_bytes(sources - 1, rsr.at[k, ch], cols(ch))
            total = src[g, :, cols(ch)].astype(F32)
            for d in range(1, sources):
                total = total + buf[d, :, cols(ch)].astype(F32)
            return total

        def ag_send(k, ref, ch):
            for dy, dx in PEERS:
                remote(
                    ref.at[g, :, cols(ch)], ref.at[g, :, cols(ch)],
                    sent.at[3 + k], agr.at[k, ch], dev_dp(dy, dx),
                ).start()

        class Gather:
            def __init__(self, buf, send, recv):
                self.buf, self.send, self.recv = buf, send, recv

            def start(self):
                for p, d in enumerate(ORDER):
                    remote(
                        self.buf.at[0], self.buf.at[1 + p], self.send,
                        self.recv.at[0 if p < FIRST else 1], dev_z(d),
                    ).start()
                self.pass_on(0, 1)

            def pass_on(self, at, n):
                remote(
                    self.buf.at[pl.ds(at, n)], self.buf.at[pl.ds(8 + at, n)], self.send, self.recv.at[2], dev_core
                ).start()

            def forward(self, group):
                at, n = (1, FIRST) if group == 0 else (1 + FIRST, 7 - FIRST)
                ref = self.buf.at[pl.ds(at, n)]
                remote(ref, ref, self.send, self.recv.at[group], dev_core).wait_recv()
                self.pass_on(at, n)

            def wait(self):
                ref = self.buf.at[pl.ds(8, 8)]
                remote(ref, ref, self.send, self.recv.at[2], dev_core).wait_recv()

        gx = Gather(rx, sent.at[6], gxr)
        gs = Gather(rs, sent.at[7], gsr)

        with jax.named_scope("load_x"):
            load_part.wait()
            lx[pl.ds(0, NS)] = part[...].astype(BF16)
            rx[0] = lx[g]
            load_lab.wait()

        with jax.named_scope("barrier"):
            pl.semaphore_wait(barrier, len(everyone))
            gx.start()
            remote(lx.at[pl.ds(0, 4)], lx.at[pl.ds(8, 4)], sent.at[8], nbr.at[0], y_up).start()
            remote(lx.at[pl.ds(4, 4)], lx.at[pl.ds(12, 4)], sent.at[8], nbr.at[0], y_down).start()

        def turn(i):
            load_data(i).wait()
            data_t[:, rows_of(i)] = data[rows_of(i), :].T

        def logits(i):
            lg[i % 2] = dot_n(lx[pl.ds(0, NS)].reshape(PB, D), data_t[:, rows_of(i)])

        def squash(i):
            p = jax.nn.sigmoid(lg[i % 2])
            resid[:, rows_of(i)] = (lab[:, rows_of(i)].astype(F32) - p).astype(BF16)
            curv[:, rows_of(i)] = p * (1.0 - p)

        def collect(i):
            term = dot_n(resid[:, rows_of(i)], data[rows_of(i), :])
            if i == 0:
                acc[...] = term
            elif i < DCH - 1:
                acc[...] += term
            else:
                psb[0] = (acc[...] + term).astype(BF16).reshape(NS, SR, D)

        with jax.named_scope("score"):
            stages = (turn, logits, squash, collect)
            for step in range(DCH + len(stages) - 1):
                for k, stage in enumerate(stages):
                    if 0 <= step - k < DCH:
                        stage(step - k)
            for ch in range(NCH):
                rs_send(0, psb.at[0], rbuf.at[0], ch)

        with jax.named_scope("fwd_x"):
            gx.forward(0)
            gx.forward(1)

        with jax.named_scope("rs0"):
            for ch in range(NCH):
                score = rs_total(0, psb.at[0], rbuf.at[0], ch, NS) - part[g, :, cols(ch)] / prior_var
                own = score.astype(BF16)
                rs[0, :, cols(ch)] = own
                ls[g, :, cols(ch)] = own
            gs.start()
            for dy, dx in PEERS:
                remote(ls.at[g], ls.at[g], sent.at[3], agr.at[0, 0], dev_dp(dy, dx)).start()
            for dy, dx in OTHERS:
                remote(rs.at[0], ls.at[8 + g], sent.at[3], agr.at[0, 0], dev_other(dy, dx)).start()

        with jax.named_scope("pair_x"):
            wait_bytes(8, nbr.at[0], slice(None))
            gx.wait()
            xlow = lx[...].reshape(2 * PB, D)
            xf = xlow.astype(F32)
            left_norm = jnp.sum(xf * xf, axis=1, keepdims=True)
            right_x = rx[...].reshape(NR, D)
            rxf = right_x.astype(F32)
            right_norm = jnp.sum(rxf * rxf, axis=1, keepdims=True)
            distance = left_norm + as_row(right_norm, 2 * PB) - 2.0 * dot_t(xlow, right_x)
            kernel_val = jnp.exp(-0.5 * inv_band * distance)
            kf[...] = kernel_val
            dist[...] = distance
            kb[...] = kernel_val.astype(BF16)
            kernel_sum = jnp.sum(kernel_val, axis=1, keepdims=True)
            ksum[...] = kernel_sum
            spread[...] = kernel_sum * xf - dot_n(kb[...], right_x)

        with jax.named_scope("fwd_s"):
            gs.forward(0)
            gs.forward(1)
        with jax.named_scope("wait_s"):
            gs.wait()

        with jax.named_scope("force"):
            for ch in range(NCH):
                kernel_s = dot_n(kb[...], rs[:, :, cols(ch)].reshape(NR, CW))
                ks[:, cols(ch)] = kernel_s
                force = (kernel_s + inv_band * spread[:, cols(ch)]) / particle_count
                psf[:, :, cols(ch)] = force.astype(BF16).reshape(2 * NS, SR, CW)
                for own, dy, dx in FORCE_TO:
                    ty, tx = at_dp(dy, dx)
                    at = 0 if own else NS
                    remote(
                        psf.at[at + ty * 4 + tx, :, cols(ch)], rforce.at[at + dy * 4 + dx, :, cols(ch)],
                        sent.at[1], rsr.at[1, ch], {"yh": ty, "x": tx, "yl": yl if own else 1 - yl},
                    ).start()

        with jax.named_scope("place"):
            wait_bytes(15, agr.at[0, 0], slice(None))
            slow = ls[...].reshape(2 * PB, D)
            xlow = lx[...].reshape(2 * PB, D)
            xf = xlow.astype(F32)
            sf = slow.astype(F32)
            left_sx = jnp.sum(sf * xf, axis=1, keepdims=True)
            right_x = rx[...].reshape(NR, D)
            right_s = rs[...].reshape(NR, D)
            right_sx = jnp.sum(right_s.astype(F32) * right_x.astype(F32), axis=1, keepdims=True)
            cross = dot_t(xlow, right_s) + dot_t(slow, right_x)
            bracket = (
                dot_t(slow, right_s) + inv_band * (left_sx - cross + as_row(right_sx, 2 * PB))
                + D * inv_band - inv_band * inv_band * dist[...]
            )
            weighted = kf[...] * bracket
            wb[...] = weighted.astype(BF16)
            weighted_sum = jnp.sum(weighted, axis=1, keepdims=True)
            weighted_x = dot_n(wb[...], right_x)
            moved = (
                -inv_band * (weighted_sum * xf - weighted_x)
                + inv_band * (ksum[...] * sf - ks[...])
                - 2.0 * inv_band * inv_band * spread[...]
            ) / particle_count
            place[...] = moved[:PB]
            psp[...] = moved[PB:].astype(BF16).reshape(NS, SR, D)

        with jax.named_scope("rs1"):
            for ch in range(NCH):
                total = rs_total(1, psf, rforce, ch, 2 * NS)
                own_force[:, cols(ch)] = total
                glow[g, :, cols(ch)] = total.astype(BF16)
                ag_send(1, glow, ch)
            for dy, dx in OTHERS:
                ty, tx = at_dp(dy, dx)
                remote(
                    psp.at[ty * 4 + tx], rplace.at[dy * 4 + dx], sent.at[9], nbr.at[1],
                    {"yh": ty, "x": tx, "yl": 1 - yl},
                ).start()
        with jax.named_scope("ag1"):
            for ch in range(NCH):
                wait_bytes(NS - 1, agr.at[1, ch], cols(ch))

        with jax.named_scope("proj"):
            for i in range(DCH):
                projected = dot_n(glow[...].reshape(PB, D), data_t[:, rows_of(i)])
                resid[:, rows_of(i)] = (curv[:, rows_of(i)] * projected).astype(BF16)

        with jax.named_scope("term"):
            for ch in range(NCH):
                term = dot_n(resid[...], data[:, cols(ch)]) - place[:, cols(ch)]
                psb[1, :, :, cols(ch)] = term.astype(BF16).reshape(NS, SR, CW)
                rs_send(2, psb.at[1], rbuf.at[1], ch)

        with jax.named_scope("base"):
            wait_bytes(NS, nbr.at[1], slice(None))
            base = own_force[...] / prior_var
            for d in range(NS):
                base = base - rplace[d].astype(F32)
            own_force[...] = base

        with jax.named_scope("rs2"):
            for ch in range(NCH):
                total = rs_total(2, psb.at[1], rbuf.at[1], ch, NS) + own_force[:, cols(ch)]
                out_ref[g, :, cols(ch)] = total.astype(BF16)
                ag_send(2, out_ref, ch)
        with jax.named_scope("ag2"):
            for ch in range(NCH):
                wait_bytes(NS - 1, agr.at[2, ch], cols(ch))

        with jax.named_scope("drain"):
            for k, shares in enumerate((7, 15, 7, 15, 7, 7, 15, 15, 8, 8)):
                ref = rforce.at[pl.ds(0, shares)]
                remote(ref, ref, sent.at[k], nbr.at[0], dev_core).wait_send()

    V = pltpu.VMEM
    S = pltpu.SemaphoreType.DMA
    scratch = [
        V((data_count, D), BF16), V((NS, SR, D), F32), V((1, data_count), jnp.int32),
        V((2 * NS, SR, D), BF16), V((2 * NS, SR, D), BF16), V((PB, data_count), BF16), V((PB, data_count), F32),
        V((2, NS, SR, D), BF16), V((2 * NS, SR, D), BF16), V((NS, SR, D), BF16),
        V((2, NS, SR, D), BF16), V((2 * NS, SR, D), BF16), V((NS, SR, D), BF16), V((NS, SR, D), BF16),
        V((2 * NZ, SR, D), BF16), V((2 * NZ, SR, D), BF16),
        V((2 * PB, NR), F32), V((2 * PB, NR), F32), V((2 * PB, NR), BF16), V((2 * PB, NR), BF16),
        V((PB, D), F32), V((SR, D), F32),
        V((D, data_count), BF16), V((2, PB, DR), F32), V((PB, D), F32), V((2 * PB, D), F32), V((2 * PB, D), F32),
        V((2 * PB, 1), F32),
        S((DCH + 2,)), S((10,)), S((3, NCH)), S((3, NCH)), S((3,)), S((3,)), S((2,)),
    ]
    return kernel, scratch


def solution(mesh):
    torus = Mesh(mesh.devices.reshape(2, 4, 8, 2, 2), DP + BLK)

    def shards(particles, data_rows, labels):
        rows, feature_count = particles.shape
        kernel, scratch = make_kernel(feature_count, data_rows.shape[0], rows * 32)
        descent = pl.pallas_call(
            kernel,
            out_shape=jax.ShapeDtypeStruct((8, 16, feature_count), BF16),
            in_specs=[pl.BlockSpec(memory_space=pl.ANY)] * 3,
            out_specs=pl.BlockSpec(memory_space=pltpu.VMEM),
            scratch_shapes=scratch,
            compiler_params=pltpu.CompilerParams(
                collective_id=0, has_side_effects=True, vmem_limit_bytes=44 * 1024 * 1024
            ),
        )(*[pltpu.with_memory_space_constraint(v, pltpu.HBM) for v in (particles.reshape(8, 16, feature_count), data_rows, labels.reshape(1, -1))])
        return descent.reshape(rows, feature_count).astype(F32)

    return jax.shard_map(
        shards,
        mesh=torus,
        in_specs=(P(BLK, None), P(DP, None), P(DP)),
        out_specs=P(BLK, None),
        check_vma=False,
    )
```

```python
import jax
import jax.numpy as jnp
from jax import lax
from jax.experimental import pallas as pl
from jax.experimental.pallas import tpu as pltpu
from jax.sharding import Mesh
from jax.sharding import PartitionSpec as P

DP = ("yh", "x")
BLK = ("z", "yl", "c")
prior_var = 4.0
NCH = 2
F32 = jnp.float32
BF16 = jnp.bfloat16

PEERS = ((1, 2), (1, 1), (1, 3), (0, 2), (1, 0), (0, 1), (0, 3))

OTHERS = ((0, 2), (1, 2), (0, 1), (1, 1), (0, 3), (1, 3), (1, 0), (0, 0))
FORCE_TO = (
    (1, 1, 2), (0, 0, 2), (0, 1, 2), (1, 1, 1), (1, 1, 3), (0, 0, 1), (0, 1, 1), (0, 0, 3),
    (0, 1, 3), (1, 0, 2), (1, 1, 0), (0, 1, 0), (0, 0, 0), (1, 0, 1), (1, 0, 3),
)
ORDER = (4, 3, 5, 2, 6, 1, 7)
FIRST = 3


def dot_t(a, b):
    return lax.dot_general(a, b, (((1,), (1,)), ((), ())), preferred_element_type=F32)


def dot_n(a, b):
    return lax.dot_general(a, b, (((1,), (0,)), ((), ())), preferred_element_type=F32)


def as_row(col, rows):
    return jnp.broadcast_to(col, (col.shape[0], rows)).T


def make_kernel(feature_count, data_count, particle_count):
    D = feature_count
    inv_band = 1.0 / D
    SR = 16
    NS = 8
    PB = SR * NS
    NZ = 8
    NR = 2 * NZ * SR
    CW = D // NCH
    DCH = 8
    DR = data_count // DCH

    def kernel(
        part_hbm, data_hbm, lab_hbm, out_ref,
        data, part, lab, lx, ls, resid, curv, psb, psf, psp, rbuf, rforce, rplace, glow, rx, rs,
        kf, dist, kb, wb, place, own_force, data_t, lg, acc, ks, spread, ksum,
        load_sem, sent, rsr, agr, gxr, gsr, nbr,
    ):
        yh, x = lax.axis_index("yh"), lax.axis_index("x")
        z, yl, c = lax.axis_index("z"), lax.axis_index("yl"), lax.axis_index("c")
        g = yh * 4 + x
        y = yh * 2 + yl

        def at_dp(dy, dx):
            return lax.rem(yh + dy, 2), lax.rem(x + dx, 4)

        def dev_dp(dy, dx):
            ty, tx = at_dp(dy, dx)
            return {"yh": ty, "x": tx}

        def dev_other(dy, dx):
            return {**dev_dp(dy, dx), "yl": 1 - yl}

        def dev_z(d):
            return {"z": lax.rem(z + d, NZ)}

        def dev_y(t):
            return {"yh": t // 2, "yl": lax.rem(t, 2)}

        y_up, y_down = dev_y(lax.rem(y + 1, 4)), dev_y(lax.rem(y + 3, 4))
        dev_core = {"c": 1 - c}
        everyone = (
            [dev_dp(*p) for p in PEERS] + [dev_other(*p) for p in OTHERS]
            + [dev_z(d) for d in range(1, NZ)] + [dev_core]
        )
        barrier = pltpu.get_barrier_semaphore()
        for dev in everyone:
            pl.semaphore_signal(barrier, inc=1, device_id=dev, device_id_type=pl.DeviceIdType.MESH)

        load_part = pltpu.make_async_copy(part_hbm, part, load_sem.at[DCH])
        load_lab = pltpu.make_async_copy(lab_hbm, lab, load_sem.at[DCH + 1])
        load_part.start()
        load_lab.start()

        def rows_of(i):
            return pl.ds(i * DR, DR)

        def load_data(i):
            return pltpu.make_async_copy(data_hbm.at[rows_of(i)], data.at[rows_of(i)], load_sem.at[i])

        for i in range(DCH):
            load_data(i).start()

        def remote(src, dst, ssem, rsem, dev):
            return pltpu.make_async_remote_copy(
                src_ref=src, dst_ref=dst, send_sem=ssem, recv_sem=rsem,
                device_id=dev, device_id_type=pl.DeviceIdType.MESH,
            )

        def cols(ch):
            return pl.ds(ch * CW, CW)

        def wait_bytes(shares, rsem, width):
            ref = rforce.at[pl.ds(0, shares), :, width]
            remote(ref, ref, sent.at[0], rsem, dev_core).wait_recv()

        def rs_send(k, src, dst, ch):
            for dy, dx in PEERS:
                ty, tx = at_dp(dy, dx)
                remote(
                    src.at[ty * 4 + tx, :, cols(ch)], dst.at[dy * 4 + dx, :, cols(ch)],
                    sent.at[k], rsr.at[k, ch], {"yh": ty, "x": tx},
                ).start()

        def rs_total(k, src, buf, ch, sources):
            wait_bytes(sources - 1, rsr.at[k, ch], cols(ch))
            total = src[g, :, cols(ch)].astype(F32)
            for d in range(1, sources):
                total = total + buf[d, :, cols(ch)].astype(F32)
            return total

        def ag_send(k, ref, ch):
            for dy, dx in PEERS:
                remote(
                    ref.at[g, :, cols(ch)], ref.at[g, :, cols(ch)],
                    sent.at[3 + k], agr.at[k, ch], dev_dp(dy, dx),
                ).start()

        class Gather:
            def __init__(self, buf, send, recv):
                self.buf, self.send, self.recv = buf, send, recv

            def start(self):
                for p, d in enumerate(ORDER):
                    remote(
                        self.buf.at[0], self.buf.at[1 + p], self.send,
                        self.recv.at[0 if p < FIRST else 1], dev_z(d),
                    ).start()
                self.pass_on(0, 1)

            def pass_on(self, at, n):
                remote(
                    self.buf.at[pl.ds(at, n)], self.buf.at[pl.ds(8 + at, n)], self.send, self.recv.at[2], dev_core
                ).start()

            def forward(self, group):
                at, n = (1, FIRST) if group == 0 else (1 + FIRST, 7 - FIRST)
                ref = self.buf.at[pl.ds(at, n)]
                remote(ref, ref, self.send, self.recv.at[group], dev_core).wait_recv()
                self.pass_on(at, n)

            def wait(self):
                ref = self.buf.at[pl.ds(8, 8)]
                remote(ref, ref, self.send, self.recv.at[2], dev_core).wait_recv()

        gx = Gather(rx, sent.at[6], gxr)
        gs = Gather(rs, sent.at[7], gsr)

        with jax.named_scope("load_x"):
            load_part.wait()
            lx[pl.ds(0, NS)] = part[...].astype(BF16)
            rx[0] = lx[g]
            load_lab.wait()

        def turn(i):
            if i % 2 == 0:
                load_data(i).wait()
                load_data(i + 1).wait()
            data_t[:, rows_of(i)] = data[rows_of(i), :].T

        def logits(i):
            lg[i % 2] = dot_n(lx[pl.ds(0, NS)].reshape(PB, D), data_t[:, rows_of(i)])

        def squash(i):
            p = jax.nn.sigmoid(lg[i % 2])
            resid[:, rows_of(i)] = (lab[:, rows_of(i)].astype(F32) - p).astype(BF16)
            curv[:, rows_of(i)] = p * (1.0 - p)

        def collect(i):
            term = dot_n(resid[:, rows_of(i)], data[rows_of(i), :])
            if i == 0:
                acc[...] = term
            elif i < DCH - 1:
                acc[...] += term
            else:
                psb[0] = (acc[...] + term).astype(BF16).reshape(NS, SR, D)

        with jax.named_scope("score"):
            stages = (turn, logits, squash, collect)
            for step in range(DCH + len(stages) - 1):
                if step == 2:
                    with jax.named_scope("barrier"):
                        pl.semaphore_wait(barrier, len(everyone))
                        gx.start()
                        remote(lx.at[pl.ds(0, 4)], lx.at[pl.ds(8, 4)], sent.at[8], nbr.at[0], y_up).start()
                        remote(lx.at[pl.ds(4, 4)], lx.at[pl.ds(12, 4)], sent.at[8], nbr.at[0], y_down).start()
                for k, stage in enumerate(stages):
                    if 0 <= step - k < DCH:
                        stage(step - k)
            for ch in range(NCH):
                rs_send(0, psb.at[0], rbuf.at[0], ch)

        with jax.named_scope("rs0"):
            for ch in range(NCH):
                score = rs_total(0, psb.at[0], rbuf.at[0], ch, NS) - part[g, :, cols(ch)] / prior_var
                own = score.astype(BF16)
                rs[0, :, cols(ch)] = own
                ls[g, :, cols(ch)] = own
            gs.start()
            for dy, dx in PEERS:
                remote(ls.at[g], ls.at[g], sent.at[3], agr.at[0, 0], dev_dp(dy, dx)).start()
            for dy, dx in OTHERS:
                remote(rs.at[0], ls.at[8 + g], sent.at[3], agr.at[0, 0], dev_other(dy, dx)).start()

        with jax.named_scope("fwd_x"):
            gx.forward(0)
            gx.forward(1)

        with jax.named_scope("pair_x"):
            wait_bytes(8, nbr.at[0], slice(None))
            gx.wait()
            xlow = lx[...].reshape(2 * PB, D)
            xf = xlow.astype(F32)
            left_norm = jnp.sum(xf * xf, axis=1, keepdims=True)
            right_x = rx[...].reshape(NR, D)
            rxf = right_x.astype(F32)
            right_norm = jnp.sum(rxf * rxf, axis=1, keepdims=True)
            distance = left_norm + as_row(right_norm, 2 * PB) - 2.0 * dot_t(xlow, right_x)
            kernel_val = jnp.exp(-0.5 * inv_band * distance)
            kf[...] = kernel_val
            dist[...] = distance
            kb[...] = kernel_val.astype(BF16)
            kernel_sum = jnp.sum(kernel_val, axis=1, keepdims=True)
            ksum[...] = kernel_sum
            spread[...] = kernel_sum * xf - dot_n(kb[...], right_x)

        with jax.named_scope("fwd_s"):
            gs.forward(0)
            gs.forward(1)
        with jax.named_scope("wait_s"):
            gs.wait()

        with jax.named_scope("force"):
            for ch in range(NCH):
                kernel_s = dot_n(kb[...], rs[:, :, cols(ch)].reshape(NR, CW))
                ks[:, cols(ch)] = kernel_s
                force = (kernel_s + inv_band * spread[:, cols(ch)]) / particle_count
                psf[:, :, cols(ch)] = force.astype(BF16).reshape(2 * NS, SR, CW)
                for own, dy, dx in FORCE_TO:
                    ty, tx = at_dp(dy, dx)
                    at = 0 if own else NS
                    remote(
                        psf.at[at + ty * 4 + tx, :, cols(ch)], rforce.at[at + dy * 4 + dx, :, cols(ch)],
                        sent.at[1], rsr.at[1, ch], {"yh": ty, "x": tx, "yl": yl if own else 1 - yl},
                    ).start()

        with jax.named_scope("place"):
            wait_bytes(15, agr.at[0, 0], slice(None))
            slow = ls[...].reshape(2 * PB, D)
            xlow = lx[...].reshape(2 * PB, D)
            xf = xlow.astype(F32)
            sf = slow.astype(F32)
            left_sx = jnp.sum(sf * xf, axis=1, keepdims=True)
            right_x = rx[...].reshape(NR, D)
            right_s = rs[...].reshape(NR, D)
            right_sx = jnp.sum(right_s.astype(F32) * right_x.astype(F32), axis=1, keepdims=True)
            cross = dot_t(xlow, right_s) + dot_t(slow, right_x)
            bracket = (
                dot_t(slow, right_s) + inv_band * (left_sx - cross + as_row(right_sx, 2 * PB))
                + D * inv_band - inv_band * inv_band * dist[...]
            )
            weighted = kf[...] * bracket
            wb[...] = weighted.astype(BF16)
            weighted_sum = jnp.sum(weighted, axis=1, keepdims=True)
            weighted_x = dot_n(wb[...], right_x)
            moved = (
                -inv_band * (weighted_sum * xf - weighted_x)
                + inv_band * (ksum[...] * sf - ks[...])
                - 2.0 * inv_band * inv_band * spread[...]
            ) / particle_count
            place[...] = moved[:PB]
            psp[...] = moved[PB:].astype(BF16).reshape(NS, SR, D)

        with jax.named_scope("rs1"):
            for ch in range(NCH):
                total = rs_total(1, psf, rforce, ch, 2 * NS)
                own_force[:, cols(ch)] = total
                glow[g, :, cols(ch)] = total.astype(BF16)
                ag_send(1, glow, ch)
            remote(psp.at[pl.ds(0, 4)], rplace.at[pl.ds(0, 4)], sent.at[9], nbr.at[1], y_up).start()
            remote(psp.at[pl.ds(4, 4)], rplace.at[pl.ds(4, 4)], sent.at[9], nbr.at[1], y_down).start()
        with jax.named_scope("ag1"):
            for ch in range(NCH):
                wait_bytes(NS - 1, agr.at[1, ch], cols(ch))

        with jax.named_scope("proj"):
            for i in range(DCH):
                projected = dot_n(glow[...].reshape(PB, D), data_t[:, rows_of(i)])
                resid[:, rows_of(i)] = (curv[:, rows_of(i)] * projected).astype(BF16)

        with jax.named_scope("term"):
            for ch in range(NCH):
                term = dot_n(resid[...], data[:, cols(ch)]) - place[:, cols(ch)]
                if ch == 0:
                    acc[:, cols(ch)] = term
                    wait_bytes(NS, nbr.at[1], slice(None))
                    term = acc[:, cols(ch)]
                term = term - rplace[:, :, cols(ch)].reshape(PB, CW).astype(F32)
                psb[1, :, :, cols(ch)] = term.astype(BF16).reshape(NS, SR, CW)
                rs_send(2, psb.at[1], rbuf.at[1], ch)

        with jax.named_scope("rs2"):
            for ch in range(NCH):
                total = rs_total(2, psb.at[1], rbuf.at[1], ch, NS) + own_force[:, cols(ch)] / prior_var
                out_ref[g, :, cols(ch)] = total.astype(BF16)
                ag_send(2, out_ref, ch)
        with jax.named_scope("ag2"):
            for ch in range(NCH):
                wait_bytes(NS - 1, agr.at[2, ch], cols(ch))

        with jax.named_scope("drain"):
            for k, shares in enumerate((7, 15, 7, 15, 7, 7, 15, 15, 8, 8)):
                ref = rforce.at[pl.ds(0, shares)]
                remote(ref, ref, sent.at[k], nbr.at[0], dev_core).wait_send()

    V = pltpu.VMEM
    S = pltpu.SemaphoreType.DMA
    scratch = [
        V((data_count, D), BF16), V((NS, SR, D), F32), V((1, data_count), jnp.int32),
        V((2 * NS, SR, D), BF16), V((2 * NS, SR, D), BF16), V((PB, data_count), BF16), V((PB, data_count), F32),
        V((2, NS, SR, D), BF16), V((2 * NS, SR, D), BF16), V((NS, SR, D), BF16),
        V((2, NS, SR, D), BF16), V((2 * NS, SR, D), BF16), V((NS, SR, D), BF16), V((NS, SR, D), BF16),
        V((2 * NZ, SR, D), BF16), V((2 * NZ, SR, D), BF16),
        V((2 * PB, NR), F32), V((2 * PB, NR), F32), V((2 * PB, NR), BF16), V((2 * PB, NR), BF16),
        V((PB, D), F32), V((SR, D), F32),
        V((D, data_count), BF16), V((2, PB, DR), F32), V((PB, D), F32), V((2 * PB, D), F32), V((2 * PB, D), F32),
        V((2 * PB, 1), F32),
        S((DCH + 2,)), S((10,)), S((3, NCH)), S((3, NCH)), S((3,)), S((3,)), S((2,)),
    ]
    return kernel, scratch


def solution(mesh):
    torus = Mesh(mesh.devices.reshape(2, 4, 8, 2, 2), DP + BLK)

    def shards(particles, data_rows, labels):
        rows, feature_count = particles.shape
        kernel, scratch = make_kernel(feature_count, data_rows.shape[0], rows * 32)
        descent = pl.pallas_call(
            kernel,
            out_shape=jax.ShapeDtypeStruct((8, 16, feature_count), BF16),
            in_specs=[pl.BlockSpec(memory_space=pl.ANY)] * 3,
            out_specs=pl.BlockSpec(memory_space=pltpu.VMEM),
            scratch_shapes=scratch,
            compiler_params=pltpu.CompilerParams(
                collective_id=0, has_side_effects=True, vmem_limit_bytes=44 * 1024 * 1024
            ),
        )(*[pltpu.with_memory_space_constraint(v, pltpu.HBM) for v in (particles.reshape(8, 16, feature_count), data_rows, labels.reshape(1, -1))])
        return descent.reshape(rows, feature_count).astype(F32)

    return jax.shard_map(
        shards,
        mesh=torus,
        in_specs=(P(BLK, None), P(DP, None), P(DP)),
        out_specs=P(BLK, None),
        check_vma=False,
    )
```

```python
import jax
import jax.numpy as jnp
from jax import lax
from jax.experimental import pallas as pl
from jax.experimental.pallas import tpu as pltpu
from jax.sharding import Mesh
from jax.sharding import PartitionSpec as P

DP = ("yh", "x")
BLK = ("z", "yl", "c")
prior_var = 4.0
NCH = 2
F32 = jnp.float32
BF16 = jnp.bfloat16

PEERS = ((1, 2), (1, 1), (1, 3), (0, 2), (1, 0), (0, 1), (0, 3))

OTHERS = ((0, 2), (1, 2), (0, 1), (1, 1), (0, 3), (1, 3), (1, 0), (0, 0))
FORCE_TO = (
    (1, 1, 2), (0, 0, 2), (0, 1, 2), (1, 1, 1), (1, 1, 3), (0, 0, 1), (0, 1, 1), (0, 0, 3),
    (0, 1, 3), (1, 0, 2), (1, 1, 0), (0, 1, 0), (0, 0, 0), (1, 0, 1), (1, 0, 3),
)
ORDER = (4, 3, 5, 2, 6, 1, 7)
FIRST = 3


def dot_t(a, b):
    return lax.dot_general(a, b, (((1,), (1,)), ((), ())), preferred_element_type=F32)


def dot_n(a, b):
    return lax.dot_general(a, b, (((1,), (0,)), ((), ())), preferred_element_type=F32)


def as_row(col, rows):
    return jnp.broadcast_to(col, (col.shape[0], rows)).T


def make_kernel(feature_count, data_count, particle_count):
    D = feature_count
    inv_band = 1.0 / D
    SR = 16
    NS = 8
    PB = SR * NS
    NZ = 8
    NR = 2 * NZ * SR
    CW = D // NCH
    DCH = 16
    GROUPS = ((0, 4), (4, 4), (8, 4), (12, 2), (14, 2))
    DR = data_count // DCH

    def kernel(
        part_hbm, data_hbm, lab_hbm, out_ref,
        data, part, lab, lx, ls, resid, curv, psb, psf, psp, rbuf, rforce, rplace, glow, rx, rs,
        kf, dist, kb, wb, place, own_force, data_t, lg, acc, ks, spread, ksum,
        load_sem, sent, rsr, agr, gxr, gsr, nbr,
    ):
        yh, x = lax.axis_index("yh"), lax.axis_index("x")
        z, yl, c = lax.axis_index("z"), lax.axis_index("yl"), lax.axis_index("c")
        g = yh * 4 + x
        y = yh * 2 + yl

        def at_dp(dy, dx):
            return lax.rem(yh + dy, 2), lax.rem(x + dx, 4)

        def dev_dp(dy, dx):
            ty, tx = at_dp(dy, dx)
            return {"yh": ty, "x": tx}

        def dev_other(dy, dx):
            return {**dev_dp(dy, dx), "yl": 1 - yl}

        def dev_z(d):
            return {"z": lax.rem(z + d, NZ)}

        def dev_y(t):
            return {"yh": t // 2, "yl": lax.rem(t, 2)}

        y_up, y_down = dev_y(lax.rem(y + 1, 4)), dev_y(lax.rem(y + 3, 4))
        dev_core = {"c": 1 - c}
        everyone = (
            [dev_dp(*p) for p in PEERS] + [dev_other(*p) for p in OTHERS]
            + [dev_z(d) for d in range(1, NZ)] + [dev_core]
        )
        barrier = pltpu.get_barrier_semaphore()
        for dev in everyone:
            pl.semaphore_signal(barrier, inc=1, device_id=dev, device_id_type=pl.DeviceIdType.MESH)

        load_part = pltpu.make_async_copy(part_hbm, part, load_sem.at[len(GROUPS)])
        load_lab = pltpu.make_async_copy(lab_hbm, lab, load_sem.at[len(GROUPS) + 1])
        load_part.start()
        load_lab.start()

        def rows_of(i):
            return pl.ds(i * DR, DR)

        def load_data(i):
            rows = pl.ds(GROUPS[i][0] * DR, GROUPS[i][1] * DR)
            return pltpu.make_async_copy(data_hbm.at[rows], data.at[rows], load_sem.at[i])

        for i in range(len(GROUPS)):
            load_data(i).start()

        def remote(src, dst, ssem, rsem, dev):
            return pltpu.make_async_remote_copy(
                src_ref=src, dst_ref=dst, send_sem=ssem, recv_sem=rsem,
                device_id=dev, device_id_type=pl.DeviceIdType.MESH,
            )

        def cols(ch):
            return pl.ds(ch * CW, CW)

        def wait_bytes(shares, rsem, width):
            ref = rforce.at[pl.ds(0, shares), :, width]
            remote(ref, ref, sent.at[0], rsem, dev_core).wait_recv()

        def rs_send(k, src, dst, ch):
            for dy, dx in PEERS:
                ty, tx = at_dp(dy, dx)
                remote(
                    src.at[ty * 4 + tx, :, cols(ch)], dst.at[dy * 4 + dx, :, cols(ch)],
                    sent.at[k], rsr.at[k, ch], {"yh": ty, "x": tx},
                ).start()

        def rs_total(k, src, buf, ch, sources):
            wait_bytes(sources - 1, rsr.at[k, ch], cols(ch))
            total = src[g, :, cols(ch)].astype(F32)
            for d in range(1, sources):
                total = total + buf[d, :, cols(ch)].astype(F32)
            return total

        def ag_send(k, ref, ch):
            for dy, dx in PEERS:
                remote(
                    ref.at[g, :, cols(ch)], ref.at[g, :, cols(ch)],
                    sent.at[3 + k], agr.at[k, ch], dev_dp(dy, dx),
                ).start()

        class Gather:
            def __init__(self, buf, send, recv):
                self.buf, self.send, self.recv = buf, send, recv

            def start(self, at=slice(None)):
                for p, d in enumerate(ORDER):
                    remote(
                        self.buf.at[0, :, at], self.buf.at[1 + p, :, at], self.send,
                        self.recv.at[0 if p < FIRST else 1], dev_z(d),
                    ).start()
                remote(self.buf.at[0, :, at], self.buf.at[8, :, at], self.send, self.recv.at[2], dev_core).start()

            def pass_on(self, at, n):
                remote(
                    self.buf.at[pl.ds(at, n)], self.buf.at[pl.ds(8 + at, n)], self.send, self.recv.at[2], dev_core
                ).start()

            def forward(self, group):
                at, n = (1, FIRST) if group == 0 else (1 + FIRST, 7 - FIRST)
                ref = self.buf.at[pl.ds(at, n)]
                remote(ref, ref, self.send, self.recv.at[group], dev_core).wait_recv()
                self.pass_on(at, n)

            def wait(self):
                ref = self.buf.at[pl.ds(8, 8)]
                remote(ref, ref, self.send, self.recv.at[2], dev_core).wait_recv()

        gx = Gather(rx, sent.at[6], gxr)
        gs = Gather(rs, sent.at[7], gsr)

        with jax.named_scope("load_x"):
            load_part.wait()
            lx[pl.ds(0, NS)] = part[...].astype(BF16)
            rx[0] = lx[g]
            load_lab.wait()

        def turn(i):
            for k, (first, _) in enumerate(GROUPS):
                if i == first:
                    load_data(k).wait()
            data_t[:, rows_of(i)] = data[rows_of(i), :].T

        def logits(i):
            lg[i % 2] = dot_n(lx[pl.ds(0, NS)].reshape(PB, D), data_t[:, rows_of(i)])

        def squash(i):
            p = jax.nn.sigmoid(lg[i % 2])
            resid[:, rows_of(i)] = (lab[:, rows_of(i)].astype(F32) - p).astype(BF16)
            curv[:, rows_of(i)] = p * (1.0 - p)

        def collect(i):
            term = dot_n(resid[:, rows_of(i)], data[rows_of(i), :])
            if i == 0:
                acc[...] = term
            elif i < DCH - 1:
                acc[...] += term
            else:
                psb[0] = (acc[...] + term).astype(BF16).reshape(NS, SR, D)

        with jax.named_scope("score"):
            stages = (turn, logits, squash, collect)
            for step in range(DCH + len(stages) - 1):
                if step == 4:
                    with jax.named_scope("barrier"):
                        pl.semaphore_wait(barrier, len(everyone))
                        gx.start()
                        remote(lx.at[pl.ds(0, 4)], lx.at[pl.ds(8, 4)], sent.at[8], nbr.at[0], y_up).start()
                        remote(lx.at[pl.ds(4, 4)], lx.at[pl.ds(12, 4)], sent.at[8], nbr.at[0], y_down).start()
                for k, stage in enumerate(stages):
                    if 0 <= step - k < DCH:
                        stage(step - k)
            for ch in range(NCH):
                rs_send(0, psb.at[0], rbuf.at[0], ch)

        with jax.named_scope("rs0"):
            for ch in range(NCH):
                score = rs_total(0, psb.at[0], rbuf.at[0], ch, NS) - part[g, :, cols(ch)] / prior_var
                own = score.astype(BF16)
                rs[0, :, cols(ch)] = own
                ls[g, :, cols(ch)] = own
                gs.start(cols(ch))
            for dy, dx in PEERS:
                remote(ls.at[g], ls.at[g], sent.at[3], agr.at[0, 0], dev_dp(dy, dx)).start()
            for dy, dx in OTHERS:
                remote(rs.at[0], ls.at[8 + g], sent.at[3], agr.at[0, 0], dev_other(dy, dx)).start()

        with jax.named_scope("fwd_x"):
            gx.forward(0)
            gx.forward(1)

        with jax.named_scope("pair_x"):
            wait_bytes(8, nbr.at[0], slice(None))
            gx.wait()
            xlow = lx[...].reshape(2 * PB, D)
            xf = xlow.astype(F32)
            left_norm = jnp.sum(xf * xf, axis=1, keepdims=True)
            right_x = rx[...].reshape(NR, D)
            rxf = right_x.astype(F32)
            right_norm = jnp.sum(rxf * rxf, axis=1, keepdims=True)
            distance = left_norm + as_row(right_norm, 2 * PB) - 2.0 * dot_t(xlow, right_x)
            kernel_val = jnp.exp(-0.5 * inv_band * distance)
            kf[...] = kernel_val
            dist[...] = distance
            kb[...] = kernel_val.astype(BF16)
            kernel_sum = jnp.sum(kernel_val, axis=1, keepdims=True)
            ksum[...] = kernel_sum
            spread[...] = kernel_sum * xf - dot_n(kb[...], right_x)

        with jax.named_scope("fwd_s"):
            gs.forward(0)
            gs.forward(1)
        with jax.named_scope("wait_s"):
            gs.wait()

        with jax.named_scope("force"):
            for ch in range(NCH):
                kernel_s = dot_n(kb[...], rs[:, :, cols(ch)].reshape(NR, CW))
                ks[:, cols(ch)] = kernel_s
                force = (kernel_s + inv_band * spread[:, cols(ch)]) / particle_count
                psf[:, :, cols(ch)] = force.astype(BF16).reshape(2 * NS, SR, CW)
                for own, dy, dx in FORCE_TO:
                    ty, tx = at_dp(dy, dx)
                    at = 0 if own else NS
                    remote(
                        psf.at[at + ty * 4 + tx, :, cols(ch)], rforce.at[at + dy * 4 + dx, :, cols(ch)],
                        sent.at[1], rsr.at[1, ch], {"yh": ty, "x": tx, "yl": yl if own else 1 - yl},
                    ).start()

        with jax.named_scope("place"):
            wait_bytes(15, agr.at[0, 0], slice(None))
            slow = ls[...].reshape(2 * PB, D)
            xlow = lx[...].reshape(2 * PB, D)
            xf = xlow.astype(F32)
            sf = slow.astype(F32)
            left_sx = jnp.sum(sf * xf, axis=1, keepdims=True)
            right_x = rx[...].reshape(NR, D)
            right_s = rs[...].reshape(NR, D)
            right_sx = jnp.sum(right_s.astype(F32) * right_x.astype(F32), axis=1, keepdims=True)
            cross = dot_t(xlow, right_s) + dot_t(slow, right_x)
            bracket = (
                dot_t(slow, right_s) + inv_band * (left_sx - cross + as_row(right_sx, 2 * PB))
                + D * inv_band - inv_band * inv_band * dist[...]
            )
            weighted = kf[...] * bracket
            wb[...] = weighted.astype(BF16)
            weighted_sum = jnp.sum(weighted, axis=1, keepdims=True)
            weighted_x = dot_n(wb[...], right_x)
            moved = (
                -inv_band * (weighted_sum * xf - weighted_x)
                + inv_band * (ksum[...] * sf - ks[...])
                - 2.0 * inv_band * inv_band * spread[...]
            ) / particle_count
            place[...] = moved[:PB]
            psp[...] = moved[PB:].astype(BF16).reshape(NS, SR, D)

        with jax.named_scope("rs1"):
            for ch in range(NCH):
                total = rs_total(1, psf, rforce, ch, 2 * NS)
                own_force[:, cols(ch)] = total
                glow[g, :, cols(ch)] = total.astype(BF16)
                ag_send(1, glow, ch)
            remote(psp.at[pl.ds(0, 4)], rplace.at[pl.ds(0, 4)], sent.at[9], nbr.at[1], y_up).start()
            remote(psp.at[pl.ds(4, 4)], rplace.at[pl.ds(4, 4)], sent.at[9], nbr.at[1], y_down).start()
        with jax.named_scope("ag1"):
            for ch in range(NCH):
                wait_bytes(NS - 1, agr.at[1, ch], cols(ch))

        with jax.named_scope("proj"):
            for i in range(8):
                rows = pl.ds(i * (data_count // 8), data_count // 8)
                projected = dot_n(glow[...].reshape(PB, D), data_t[:, rows])
                resid[:, rows] = (curv[:, rows] * projected).astype(BF16)

        with jax.named_scope("term"):
            for ch in range(NCH):
                term = dot_n(resid[...], data[:, cols(ch)]) - place[:, cols(ch)]
                if ch == 0:
                    acc[:, cols(ch)] = term
                    wait_bytes(NS, nbr.at[1], slice(None))
                    term = acc[:, cols(ch)]
                term = term - rplace[:, :, cols(ch)].reshape(PB, CW).astype(F32)
                psb[1, :, :, cols(ch)] = term.astype(BF16).reshape(NS, SR, CW)
                rs_send(2, psb.at[1], rbuf.at[1], ch)

        with jax.named_scope("rs2"):
            for ch in range(NCH):
                total = rs_total(2, psb.at[1], rbuf.at[1], ch, NS) + own_force[:, cols(ch)] / prior_var
                out_ref[g, :, cols(ch)] = total.astype(BF16)
                ag_send(2, out_ref, ch)
        with jax.named_scope("ag2"):
            for ch in range(NCH):
                wait_bytes(NS - 1, agr.at[2, ch], cols(ch))

        with jax.named_scope("drain"):
            for k, shares in enumerate((7, 15, 7, 15, 7, 7, 15, 15, 8, 8)):
                ref = rforce.at[pl.ds(0, shares)]
                remote(ref, ref, sent.at[k], nbr.at[0], dev_core).wait_send()

    V = pltpu.VMEM
    S = pltpu.SemaphoreType.DMA
    scratch = [
        V((data_count, D), BF16), V((NS, SR, D), F32), V((1, data_count), jnp.int32),
        V((2 * NS, SR, D), BF16), V((2 * NS, SR, D), BF16), V((PB, data_count), BF16), V((PB, data_count), F32),
        V((2, NS, SR, D), BF16), V((2 * NS, SR, D), BF16), V((NS, SR, D), BF16),
        V((2, NS, SR, D), BF16), V((2 * NS, SR, D), BF16), V((NS, SR, D), BF16), V((NS, SR, D), BF16),
        V((2 * NZ, SR, D), BF16), V((2 * NZ, SR, D), BF16),
        V((2 * PB, NR), F32), V((2 * PB, NR), F32), V((2 * PB, NR), BF16), V((2 * PB, NR), BF16),
        V((PB, D), F32), V((SR, D), F32),
        V((D, data_count), BF16), V((2, PB, DR), F32), V((PB, D), F32), V((2 * PB, D), F32), V((2 * PB, D), F32),
        V((2 * PB, 1), F32),
        S((len(GROUPS) + 2,)), S((10,)), S((3, NCH)), S((3, NCH)), S((3,)), S((3,)), S((2,)),
    ]
    return kernel, scratch


def solution(mesh):
    torus = Mesh(mesh.devices.reshape(2, 4, 8, 2, 2), DP + BLK)

    def shards(particles, data_rows, labels):
        rows, feature_count = particles.shape
        kernel, scratch = make_kernel(feature_count, data_rows.shape[0], rows * 32)
        descent = pl.pallas_call(
            kernel,
            out_shape=jax.ShapeDtypeStruct((8, 16, feature_count), BF16),
            in_specs=[pl.BlockSpec(memory_space=pl.ANY)] * 3,
            out_specs=pl.BlockSpec(memory_space=pltpu.VMEM),
            scratch_shapes=scratch,
            compiler_params=pltpu.CompilerParams(
                collective_id=0, has_side_effects=True, vmem_limit_bytes=44 * 1024 * 1024
            ),
        )(*[pltpu.with_memory_space_constraint(v, pltpu.HBM) for v in (particles.reshape(8, 16, feature_count), data_rows, labels.reshape(1, -1))])
        return descent.reshape(rows, feature_count).astype(F32)

    return jax.shard_map(
        shards,
        mesh=torus,
        in_specs=(P(BLK, None), P(DP, None), P(DP)),
        out_specs=P(BLK, None),
        check_vma=False,
    )
```

```python
import jax
import jax.numpy as jnp
from jax import lax
from jax.experimental import pallas as pl
from jax.experimental.pallas import tpu as pltpu
from jax.sharding import Mesh
from jax.sharding import PartitionSpec as P

DP = ("yh", "x")
BLK = ("z", "yl", "c")
prior_var = 4.0
NCH = 2
F32 = jnp.float32
BF16 = jnp.bfloat16

PEERS = ((1, 2), (1, 1), (1, 3), (0, 2), (1, 0), (0, 1), (0, 3))

OTHERS = ((0, 2), (1, 2), (0, 1), (1, 1), (0, 3), (1, 3), (1, 0), (0, 0))
FORCE_TO = (
    (1, 1, 2), (0, 0, 2), (0, 1, 2), (1, 1, 1), (1, 1, 3), (0, 0, 1), (0, 1, 1), (0, 0, 3),
    (0, 1, 3), (1, 0, 2), (1, 1, 0), (0, 1, 0), (0, 0, 0), (1, 0, 1), (1, 0, 3),
)
ORDER = (4, 3, 5, 2, 6, 1, 7)
FIRST = 3


def dot_t(a, b):
    return lax.dot_general(a, b, (((1,), (1,)), ((), ())), preferred_element_type=F32)


def dot_n(a, b):
    return lax.dot_general(a, b, (((1,), (0,)), ((), ())), preferred_element_type=F32)


def as_row(col, rows):
    return jnp.broadcast_to(col, (col.shape[0], rows)).T


def make_kernel(feature_count, data_count, particle_count):
    D = feature_count
    inv_band = 1.0 / D
    SR = 16
    NS = 8
    PB = SR * NS
    NZ = 8
    NR = 2 * NZ * SR
    CW = D // NCH
    DCH = 16
    GROUPS = ((0, 4), (4, 4), (8, 4), (12, 2), (14, 2))
    DR = data_count // DCH

    def kernel(
        part_hbm, data_hbm, lab_hbm, out_ref,
        data, part, lab, lx, ls, resid, curv, psb, psf, psp, rbuf, rforce, rplace, glow, rx, rs,
        kf, dist, kb, wb, place, own_force, data_t, lg, acc, ks, spread, ksum,
        load_sem, sent, rsr, agr, gxr, gsr, nbr,
    ):
        yh, x = lax.axis_index("yh"), lax.axis_index("x")
        z, yl, c = lax.axis_index("z"), lax.axis_index("yl"), lax.axis_index("c")
        g = yh * 4 + x
        y = yh * 2 + yl

        def at_dp(dy, dx):
            return lax.rem(yh + dy, 2), lax.rem(x + dx, 4)

        def dev_dp(dy, dx):
            ty, tx = at_dp(dy, dx)
            return {"yh": ty, "x": tx}

        def dev_other(dy, dx):
            return {**dev_dp(dy, dx), "yl": 1 - yl}

        def dev_z(d):
            return {"z": lax.rem(z + d, NZ)}

        def dev_y(t):
            return {"yh": t // 2, "yl": lax.rem(t, 2)}

        y_up, y_down = dev_y(lax.rem(y + 1, 4)), dev_y(lax.rem(y + 3, 4))
        dev_core = {"c": 1 - c}
        everyone = (
            [dev_dp(*p) for p in PEERS] + [dev_other(*p) for p in OTHERS]
            + [dev_z(d) for d in range(1, NZ)] + [dev_core]
        )
        barrier = pltpu.get_barrier_semaphore()
        for dev in everyone:
            pl.semaphore_signal(barrier, inc=1, device_id=dev, device_id_type=pl.DeviceIdType.MESH)

        load_part = pltpu.make_async_copy(part_hbm, part, load_sem.at[len(GROUPS)])
        load_lab = pltpu.make_async_copy(lab_hbm, lab, load_sem.at[len(GROUPS) + 1])
        load_part.start()
        load_lab.start()

        def rows_of(i):
            return pl.ds(i * DR, DR)

        def load_data(i):
            rows = pl.ds(GROUPS[i][0] * DR, GROUPS[i][1] * DR)
            return pltpu.make_async_copy(data_hbm.at[rows], data.at[rows], load_sem.at[i])

        for i in range(len(GROUPS)):
            load_data(i).start()

        def remote(src, dst, ssem, rsem, dev):
            return pltpu.make_async_remote_copy(
                src_ref=src, dst_ref=dst, send_sem=ssem, recv_sem=rsem,
                device_id=dev, device_id_type=pl.DeviceIdType.MESH,
            )

        def cols(ch):
            return pl.ds(ch * CW, CW)

        def wait_bytes(shares, rsem, width):
            ref = rforce.at[pl.ds(0, shares), :, width]
            remote(ref, ref, sent.at[0], rsem, dev_core).wait_recv()

        def rs_send(k, src, dst, ch):
            for dy, dx in PEERS:
                ty, tx = at_dp(dy, dx)
                remote(
                    src.at[ty * 4 + tx, :, cols(ch)], dst.at[dy * 4 + dx, :, cols(ch)],
                    sent.at[k], rsr.at[k, ch], {"yh": ty, "x": tx},
                ).start()

        def rs_total(k, src, buf, ch, sources):
            wait_bytes(sources - 1, rsr.at[k, ch], cols(ch))
            total = src[g, :, cols(ch)].astype(F32)
            for d in range(1, sources):
                total = total + buf[d, :, cols(ch)].astype(F32)
            return total

        def ag_send(k, ref, ch):
            for dy, dx in PEERS:
                remote(
                    ref.at[g, :, cols(ch)], ref.at[g, :, cols(ch)],
                    sent.at[3 + k], agr.at[k, ch], dev_dp(dy, dx),
                ).start()

        class Gather:
            def __init__(self, buf, send, recv):
                self.buf, self.send, self.recv = buf, send, recv

            def start(self, at=slice(None)):
                for p, d in enumerate(ORDER):
                    remote(
                        self.buf.at[0, :, at], self.buf.at[1 + p, :, at], self.send,
                        self.recv.at[0 if p < FIRST else 1], dev_z(d),
                    ).start()
                remote(self.buf.at[0, :, at], self.buf.at[8, :, at], self.send, self.recv.at[2], dev_core).start()

            def pass_on(self, at, n):
                remote(
                    self.buf.at[pl.ds(at, n)], self.buf.at[pl.ds(8 + at, n)], self.send, self.recv.at[2], dev_core
                ).start()

            def forward(self, group):
                at, n = (1, FIRST) if group == 0 else (1 + FIRST, 7 - FIRST)
                ref = self.buf.at[pl.ds(at, n)]
                remote(ref, ref, self.send, self.recv.at[group], dev_core).wait_recv()
                self.pass_on(at, n)

            def wait(self):
                ref = self.buf.at[pl.ds(8, 8)]
                remote(ref, ref, self.send, self.recv.at[2], dev_core).wait_recv()

        gx = Gather(rx, sent.at[6], gxr)
        gs = Gather(rs, sent.at[7], gsr)

        with jax.named_scope("load_x"):
            load_part.wait()
            lx[pl.ds(0, NS)] = part[...].astype(BF16)
            rx[0] = lx[g]
            load_lab.wait()

        def turn(i):
            for k, (first, _) in enumerate(GROUPS):
                if i == first:
                    load_data(k).wait()
            data_t[:, rows_of(i)] = data[rows_of(i), :].T

        def logits(i):
            lg[i % 2] = dot_n(lx[pl.ds(0, NS)].reshape(PB, D), data_t[:, rows_of(i)])

        def squash(i):
            p = jax.nn.sigmoid(lg[i % 2])
            resid[:, rows_of(i)] = (lab[:, rows_of(i)].astype(F32) - p).astype(BF16)
            curv[:, rows_of(i)] = p * (1.0 - p)

        def collect(i):
            term = dot_n(resid[:, rows_of(i)], data[rows_of(i), :])
            if i == 0:
                acc[...] = term
            elif i < DCH - 1:
                acc[...] += term
            else:
                psb[0] = (acc[...] + term).astype(BF16).reshape(NS, SR, D)

        with jax.named_scope("score"):
            stages = (turn, logits, squash, collect)
            for step in range(DCH + len(stages) - 1):
                if step == 7:
                    with jax.named_scope("barrier"):
                        pl.semaphore_wait(barrier, len(everyone))
                        gx.start()
                        remote(lx.at[pl.ds(0, 4)], lx.at[pl.ds(8, 4)], sent.at[8], nbr.at[0], y_up).start()
                        remote(lx.at[pl.ds(4, 4)], lx.at[pl.ds(12, 4)], sent.at[8], nbr.at[0], y_down).start()
                for k, stage in enumerate(stages):
                    if 0 <= step - k < DCH:
                        stage(step - k)
            for ch in range(NCH):
                rs_send(0, psb.at[0], rbuf.at[0], ch)

        with jax.named_scope("rs0"):
            for ch in range(NCH):
                score = rs_total(0, psb.at[0], rbuf.at[0], ch, NS) - part[g, :, cols(ch)] / prior_var
                own = score.astype(BF16)
                rs[0, :, cols(ch)] = own
                ls[g, :, cols(ch)] = own
                gs.start(cols(ch))
            for dy, dx in PEERS:
                remote(ls.at[g], ls.at[g], sent.at[3], agr.at[0, 0], dev_dp(dy, dx)).start()
            for dy, dx in OTHERS:
                remote(rs.at[0], ls.at[8 + g], sent.at[3], agr.at[0, 0], dev_other(dy, dx)).start()

        with jax.named_scope("fwd_x"):
            gx.forward(0)
            gx.forward(1)

        with jax.named_scope("pair_x"):
            wait_bytes(8, nbr.at[0], slice(None))
            gx.wait()
            xlow = lx[...].reshape(2 * PB, D)
            xf = xlow.astype(F32)
            left_norm = jnp.sum(xf * xf, axis=1, keepdims=True)
            right_x = rx[...].reshape(NR, D)
            rxf = right_x.astype(F32)
            right_norm = jnp.sum(rxf * rxf, axis=1, keepdims=True)
            distance = left_norm + as_row(right_norm, 2 * PB) - 2.0 * dot_t(xlow, right_x)
            kernel_val = jnp.exp(-0.5 * inv_band * distance)
            kf[...] = kernel_val
            dist[...] = distance
            kb[...] = kernel_val.astype(BF16)
            kernel_sum = jnp.sum(kernel_val, axis=1, keepdims=True)
            ksum[...] = kernel_sum
            spread[...] = kernel_sum * xf - dot_n(kb[...], right_x)

        with jax.named_scope("fwd_s"):
            gs.forward(0)
            gs.forward(1)
        with jax.named_scope("wait_s"):
            gs.wait()

        with jax.named_scope("force"):
            for ch in range(NCH):
                kernel_s = dot_n(kb[...], rs[:, :, cols(ch)].reshape(NR, CW))
                ks[:, cols(ch)] = kernel_s
                force = (kernel_s + inv_band * spread[:, cols(ch)]) / particle_count
                psf[:, :, cols(ch)] = force.astype(BF16).reshape(2 * NS, SR, CW)
                for own, dy, dx in FORCE_TO:
                    ty, tx = at_dp(dy, dx)
                    at = 0 if own else NS
                    remote(
                        psf.at[at + ty * 4 + tx, :, cols(ch)], rforce.at[at + dy * 4 + dx, :, cols(ch)],
                        sent.at[1], rsr.at[1, ch], {"yh": ty, "x": tx, "yl": yl if own else 1 - yl},
                    ).start()

        with jax.named_scope("place"):
            wait_bytes(15, agr.at[0, 0], slice(None))
            slow = ls[...].reshape(2 * PB, D)
            xlow = lx[...].reshape(2 * PB, D)
            xf = xlow.astype(F32)
            sf = slow.astype(F32)
            left_sx = jnp.sum(sf * xf, axis=1, keepdims=True)
            right_x = rx[...].reshape(NR, D)
            right_s = rs[...].reshape(NR, D)
            right_sx = jnp.sum(right_s.astype(F32) * right_x.astype(F32), axis=1, keepdims=True)
            cross = dot_t(xlow, right_s) + dot_t(slow, right_x)
            bracket = (
                dot_t(slow, right_s) + inv_band * (left_sx - cross + as_row(right_sx, 2 * PB))
                + D * inv_band - inv_band * inv_band * dist[...]
            )
            weighted = kf[...] * bracket
            wb[...] = weighted.astype(BF16)
            weighted_sum = jnp.sum(weighted, axis=1, keepdims=True)
            weighted_x = dot_n(wb[...], right_x)
            moved = (
                -inv_band * (weighted_sum * xf - weighted_x)
                + inv_band * (ksum[...] * sf - ks[...])
                - 2.0 * inv_band * inv_band * spread[...]
            ) / particle_count
            place[...] = moved[:PB]
            psp[...] = moved[PB:].astype(BF16).reshape(NS, SR, D)

        with jax.named_scope("rs1"):
            for ch in range(NCH):
                total = rs_total(1, psf, rforce, ch, 2 * NS)
                own_force[:, cols(ch)] = total
                glow[g, :, cols(ch)] = total.astype(BF16)
                ag_send(1, glow, ch)
            remote(psp.at[pl.ds(0, 4)], rplace.at[pl.ds(0, 4)], sent.at[9], nbr.at[1], y_up).start()
            remote(psp.at[pl.ds(4, 4)], rplace.at[pl.ds(4, 4)], sent.at[9], nbr.at[1], y_down).start()
        with jax.named_scope("ag1"):
            for ch in range(NCH):
                wait_bytes(NS - 1, agr.at[1, ch], cols(ch))

        with jax.named_scope("proj"):
            for i in range(8):
                rows = pl.ds(i * (data_count // 8), data_count // 8)
                projected = dot_n(glow[...].reshape(PB, D), data_t[:, rows])
                resid[:, rows] = (curv[:, rows] * projected).astype(BF16)

        with jax.named_scope("term"):
            for ch in range(NCH):
                term = dot_n(resid[...], data[:, cols(ch)]) - place[:, cols(ch)]
                if ch == 0:
                    acc[:, cols(ch)] = term
                    wait_bytes(NS, nbr.at[1], slice(None))
                    term = acc[:, cols(ch)]
                term = term - rplace[:, :, cols(ch)].reshape(PB, CW).astype(F32)
                psb[1, :, :, cols(ch)] = term.astype(BF16).reshape(NS, SR, CW)
                rs_send(2, psb.at[1], rbuf.at[1], ch)

        with jax.named_scope("rs2"):
            for ch in range(NCH):
                total = rs_total(2, psb.at[1], rbuf.at[1], ch, NS) + own_force[:, cols(ch)] / prior_var
                out_ref[g, :, cols(ch)] = total.astype(BF16)
                ag_send(2, out_ref, ch)
        with jax.named_scope("ag2"):
            for ch in range(NCH):
                wait_bytes(NS - 1, agr.at[2, ch], cols(ch))

        with jax.named_scope("drain"):
            for k, shares in enumerate((7, 15, 7, 15, 7, 7, 15, 15, 8, 8)):
                ref = rforce.at[pl.ds(0, shares)]
                remote(ref, ref, sent.at[k], nbr.at[0], dev_core).wait_send()

    V = pltpu.VMEM
    S = pltpu.SemaphoreType.DMA
    scratch = [
        V((data_count, D), BF16), V((NS, SR, D), F32), V((1, data_count), jnp.int32),
        V((2 * NS, SR, D), BF16), V((2 * NS, SR, D), BF16), V((PB, data_count), BF16), V((PB, data_count), F32),
        V((2, NS, SR, D), BF16), V((2 * NS, SR, D), BF16), V((NS, SR, D), BF16),
        V((2, NS, SR, D), BF16), V((2 * NS, SR, D), BF16), V((NS, SR, D), BF16), V((NS, SR, D), BF16),
        V((2 * NZ, SR, D), BF16), V((2 * NZ, SR, D), BF16),
        V((2 * PB, NR), F32), V((2 * PB, NR), F32), V((2 * PB, NR), BF16), V((2 * PB, NR), BF16),
        V((PB, D), F32), V((SR, D), F32),
        V((D, data_count), BF16), V((2, PB, DR), F32), V((PB, D), F32), V((2 * PB, D), F32), V((2 * PB, D), F32),
        V((2 * PB, 1), F32),
        S((len(GROUPS) + 2,)), S((10,)), S((3, NCH)), S((3, NCH)), S((3,)), S((3,)), S((2,)),
    ]
    return kernel, scratch


def solution(mesh):
    torus = Mesh(mesh.devices.reshape(2, 4, 8, 2, 2), DP + BLK)

    def shards(particles, data_rows, labels):
        rows, feature_count = particles.shape
        kernel, scratch = make_kernel(feature_count, data_rows.shape[0], rows * 32)
        descent = pl.pallas_call(
            kernel,
            out_shape=jax.ShapeDtypeStruct((8, 16, feature_count), BF16),
            in_specs=[pl.BlockSpec(memory_space=pl.ANY)] * 3,
            out_specs=pl.BlockSpec(memory_space=pltpu.VMEM),
            scratch_shapes=scratch,
            compiler_params=pltpu.CompilerParams(
                collective_id=0, has_side_effects=True, vmem_limit_bytes=44 * 1024 * 1024
            ),
        )(*[pltpu.with_memory_space_constraint(v, pltpu.HBM) for v in (particles.reshape(8, 16, feature_count), data_rows, labels.reshape(1, -1))])
        return descent.reshape(rows, feature_count).astype(F32)

    return jax.shard_map(
        shards,
        mesh=torus,
        in_specs=(P(BLK, None), P(DP, None), P(DP)),
        out_specs=P(BLK, None),
        check_vma=False,
    )
```

```python
import jax
import jax.numpy as jnp
from jax import lax
from jax.experimental import pallas as pl
from jax.experimental.pallas import tpu as pltpu
from jax.sharding import Mesh
from jax.sharding import PartitionSpec as P

DP = ("yh", "x")
BLK = ("z", "yl", "c")
prior_var = 4.0
NCH = 2
F32 = jnp.float32
BF16 = jnp.bfloat16

PEERS = ((1, 2), (1, 1), (1, 3), (0, 2), (1, 0), (0, 1), (0, 3))

OTHERS = ((0, 2), (1, 2), (0, 1), (1, 1), (0, 3), (1, 3), (1, 0), (0, 0))
FORCE_TO = (
    (1, 1, 2), (0, 1, 2), (0, 0, 2), (1, 0, 2), (1, 1, 1), (1, 1, 3), (0, 1, 1), (0, 1, 3),
    (0, 0, 1), (0, 0, 3), (1, 0, 1), (1, 0, 3), (1, 1, 0), (0, 1, 0), (0, 0, 0),
)
ORDER = (4, 3, 5, 2, 6, 1, 7)
FIRST = 3


def dot_t(a, b):
    return lax.dot_general(a, b, (((1,), (1,)), ((), ())), preferred_element_type=F32)


def dot_n(a, b):
    return lax.dot_general(a, b, (((1,), (0,)), ((), ())), preferred_element_type=F32)


def as_row(col, rows):
    return jnp.broadcast_to(col, (col.shape[0], rows)).T


def make_kernel(feature_count, data_count, particle_count):
    D = feature_count
    inv_band = 1.0 / D
    SR = 16
    NS = 8
    PB = SR * NS
    NZ = 8
    NR = 2 * NZ * SR
    CW = D // NCH
    DCH = 16
    GROUPS = ((0, 4), (4, 4), (8, 4), (12, 2), (14, 2))
    DR = data_count // DCH

    def kernel(
        part_hbm, data_hbm, lab_hbm, out_ref,
        data, part, lab, lx, ls, resid, curv, psb, psf, psp, rbuf, rforce, rplace, glow, rx, rs,
        kf, dist, kb, wb, place, own_force, data_t, lg, acc, ks, spread, ksum,
        load_sem, sent, rsr, agr, gxr, gsr, nbr,
    ):
        yh, x = lax.axis_index("yh"), lax.axis_index("x")
        z, yl, c = lax.axis_index("z"), lax.axis_index("yl"), lax.axis_index("c")
        g = yh * 4 + x
        y = yh * 2 + yl

        def at_dp(dy, dx):
            return lax.rem(yh + dy, 2), lax.rem(x + dx, 4)

        def dev_dp(dy, dx):
            ty, tx = at_dp(dy, dx)
            return {"yh": ty, "x": tx}

        def dev_other(dy, dx):
            return {**dev_dp(dy, dx), "yl": 1 - yl}

        def dev_z(d):
            return {"z": lax.rem(z + d, NZ)}

        def dev_y(t):
            return {"yh": t // 2, "yl": lax.rem(t, 2)}

        y_up, y_down = dev_y(lax.rem(y + 1, 4)), dev_y(lax.rem(y + 3, 4))
        dev_core = {"c": 1 - c}
        everyone = (
            [dev_dp(*p) for p in PEERS] + [dev_other(*p) for p in OTHERS]
            + [dev_z(d) for d in range(1, NZ)] + [dev_core]
        )
        barrier = pltpu.get_barrier_semaphore()
        for dev in everyone:
            pl.semaphore_signal(barrier, inc=1, device_id=dev, device_id_type=pl.DeviceIdType.MESH)

        load_part = pltpu.make_async_copy(part_hbm, part, load_sem.at[len(GROUPS)])
        load_lab = pltpu.make_async_copy(lab_hbm, lab, load_sem.at[len(GROUPS) + 1])
        load_part.start()
        load_lab.start()

        def rows_of(i):
            return pl.ds(i * DR, DR)

        def load_data(i):
            rows = pl.ds(GROUPS[i][0] * DR, GROUPS[i][1] * DR)
            return pltpu.make_async_copy(data_hbm.at[rows], data.at[rows], load_sem.at[i])

        for i in range(len(GROUPS)):
            load_data(i).start()

        def remote(src, dst, ssem, rsem, dev):
            return pltpu.make_async_remote_copy(
                src_ref=src, dst_ref=dst, send_sem=ssem, recv_sem=rsem,
                device_id=dev, device_id_type=pl.DeviceIdType.MESH,
            )

        def cols(ch):
            return pl.ds(ch * CW, CW)

        def wait_bytes(shares, rsem, width):
            ref = rforce.at[pl.ds(0, shares), :, width]
            remote(ref, ref, sent.at[0], rsem, dev_core).wait_recv()

        def rs_send(k, src, dst, ch):
            for dy, dx in PEERS:
                ty, tx = at_dp(dy, dx)
                remote(
                    src.at[ty * 4 + tx, :, cols(ch)], dst.at[dy * 4 + dx, :, cols(ch)],
                    sent.at[k], rsr.at[k, ch], {"yh": ty, "x": tx},
                ).start()

        def rs_total(k, src, buf, ch, sources):
            wait_bytes(sources - 1, rsr.at[k, ch], cols(ch))
            total = src[g, :, cols(ch)].astype(F32)
            for d in range(1, sources):
                total = total + buf[d, :, cols(ch)].astype(F32)
            return total

        def ag_send(k, ref, ch):
            for dy, dx in PEERS:
                remote(
                    ref.at[g, :, cols(ch)], ref.at[g, :, cols(ch)],
                    sent.at[3 + k], agr.at[k, ch], dev_dp(dy, dx),
                ).start()

        class Gather:
            def __init__(self, buf, send, recv):
                self.buf, self.send, self.recv = buf, send, recv

            def start(self, at=slice(None)):
                for p, d in enumerate(ORDER):
                    remote(
                        self.buf.at[0, :, at], self.buf.at[1 + p, :, at], self.send,
                        self.recv.at[0 if p < FIRST else 1], dev_z(d),
                    ).start()
                remote(self.buf.at[0, :, at], self.buf.at[8, :, at], self.send, self.recv.at[2], dev_core).start()

            def pass_on(self, at, n):
                remote(
                    self.buf.at[pl.ds(at, n)], self.buf.at[pl.ds(8 + at, n)], self.send, self.recv.at[2], dev_core
                ).start()

            def forward(self, group):
                at, n = (1, FIRST) if group == 0 else (1 + FIRST, 7 - FIRST)
                ref = self.buf.at[pl.ds(at, n)]
                remote(ref, ref, self.send, self.recv.at[group], dev_core).wait_recv()
                self.pass_on(at, n)

            def wait(self):
                ref = self.buf.at[pl.ds(8, 8)]
                remote(ref, ref, self.send, self.recv.at[2], dev_core).wait_recv()

        gx = Gather(rx, sent.at[6], gxr)
        gs = Gather(rs, sent.at[7], gsr)

        with jax.named_scope("load_x"):
            load_part.wait()
            lx[pl.ds(0, NS)] = part[...].astype(BF16)
            rx[0] = lx[g]
            load_lab.wait()

        def turn(i):
            for k, (first, _) in enumerate(GROUPS):
                if i == first:
                    load_data(k).wait()
            data_t[:, rows_of(i)] = data[rows_of(i), :].T

        def logits(i):
            lg[i % 2] = dot_n(lx[pl.ds(0, NS)].reshape(PB, D), data_t[:, rows_of(i)])

        def squash(i):
            p = jax.nn.sigmoid(lg[i % 2])
            resid[:, rows_of(i)] = (lab[:, rows_of(i)].astype(F32) - p).astype(BF16)
            curv[:, rows_of(i)] = p * (1.0 - p)

        def collect(i):
            term = dot_n(resid[:, rows_of(i)], data[rows_of(i), :])
            if i == 0:
                acc[...] = term
            elif i < DCH - 1:
                acc[...] += term
            else:
                psb[0] = (acc[...] + term).astype(BF16).reshape(NS, SR, D)

        with jax.named_scope("score"):
            stages = (turn, logits, squash, collect)
            for step in range(DCH + len(stages) - 1):
                if step == 7:
                    with jax.named_scope("barrier"):
                        pl.semaphore_wait(barrier, len(everyone))
                        gx.start()
                        remote(lx.at[pl.ds(0, 4)], lx.at[pl.ds(8, 4)], sent.at[8], nbr.at[0], y_up).start()
                        remote(lx.at[pl.ds(4, 4)], lx.at[pl.ds(12, 4)], sent.at[8], nbr.at[0], y_down).start()
                for k, stage in enumerate(stages):
                    if 0 <= step - k < DCH:
                        stage(step - k)
            for ch in range(NCH):
                rs_send(0, psb.at[0], rbuf.at[0], ch)

        with jax.named_scope("rs0"):
            for ch in range(NCH):
                score = rs_total(0, psb.at[0], rbuf.at[0], ch, NS) - part[g, :, cols(ch)] / prior_var
                own = score.astype(BF16)
                rs[0, :, cols(ch)] = own
                ls[g, :, cols(ch)] = own
                gs.start(cols(ch))
            for dy, dx in PEERS:
                remote(ls.at[g], ls.at[g], sent.at[3], agr.at[0, 0], dev_dp(dy, dx)).start()
            for dy, dx in OTHERS:
                remote(rs.at[0], ls.at[8 + g], sent.at[3], agr.at[0, 0], dev_other(dy, dx)).start()

        with jax.named_scope("fwd_x"):
            gx.forward(0)
            gx.forward(1)

        with jax.named_scope("pair_x"):
            wait_bytes(8, nbr.at[0], slice(None))
            gx.wait()
            xlow = lx[...].reshape(2 * PB, D)
            xf = xlow.astype(F32)
            left_norm = jnp.sum(xf * xf, axis=1, keepdims=True)
            right_x = rx[...].reshape(NR, D)
            rxf = right_x.astype(F32)
            right_norm = jnp.sum(rxf * rxf, axis=1, keepdims=True)
            distance = left_norm + as_row(right_norm, 2 * PB) - 2.0 * dot_t(xlow, right_x)
            kernel_val = jnp.exp(-0.5 * inv_band * distance)
            kf[...] = kernel_val
            dist[...] = distance
            kb[...] = kernel_val.astype(BF16)
            kernel_sum = jnp.sum(kernel_val, axis=1, keepdims=True)
            ksum[...] = kernel_sum
            spread[...] = kernel_sum * xf - dot_n(kb[...], right_x)

        with jax.named_scope("fwd_s"):
            gs.forward(0)
            gs.forward(1)
        with jax.named_scope("wait_s"):
            gs.wait()

        with jax.named_scope("force"):
            for ch in range(NCH):
                kernel_s = dot_n(kb[...], rs[:, :, cols(ch)].reshape(NR, CW))
                ks[:, cols(ch)] = kernel_s
                force = (kernel_s + inv_band * spread[:, cols(ch)]) / particle_count
                psf[:, :, cols(ch)] = force.astype(BF16).reshape(2 * NS, SR, CW)
                for own, dy, dx in FORCE_TO:
                    ty, tx = at_dp(dy, dx)
                    at = 0 if own else NS
                    remote(
                        psf.at[at + ty * 4 + tx, :, cols(ch)], rforce.at[at + dy * 4 + dx, :, cols(ch)],
                        sent.at[1], rsr.at[1, ch], {"yh": ty, "x": tx, "yl": yl if own else 1 - yl},
                    ).start()

        with jax.named_scope("place"):
            wait_bytes(15, agr.at[0, 0], slice(None))
            slow = ls[...].reshape(2 * PB, D)
            xlow = lx[...].reshape(2 * PB, D)
            xf = xlow.astype(F32)
            sf = slow.astype(F32)
            left_sx = jnp.sum(sf * xf, axis=1, keepdims=True)
            right_x = rx[...].reshape(NR, D)
            right_s = rs[...].reshape(NR, D)
            right_sx = jnp.sum(right_s.astype(F32) * right_x.astype(F32), axis=1, keepdims=True)
            cross = dot_t(xlow, right_s) + dot_t(slow, right_x)
            bracket = (
                dot_t(slow, right_s) + inv_band * (left_sx - cross + as_row(right_sx, 2 * PB))
                + D * inv_band - inv_band * inv_band * dist[...]
            )
            weighted = kf[...] * bracket
            wb[...] = weighted.astype(BF16)
            weighted_sum = jnp.sum(weighted, axis=1, keepdims=True)
            weighted_x = dot_n(wb[...], right_x)
            moved = (
                -inv_band * (weighted_sum * xf - weighted_x)
                + inv_band * (ksum[...] * sf - ks[...])
                - 2.0 * inv_band * inv_band * spread[...]
            ) / particle_count
            place[...] = moved[:PB]
            psp[...] = moved[PB:].astype(BF16).reshape(NS, SR, D)

        with jax.named_scope("rs1"):
            for ch in range(NCH):
                total = rs_total(1, psf, rforce, ch, 2 * NS)
                own_force[:, cols(ch)] = total
                glow[g, :, cols(ch)] = total.astype(BF16)
                ag_send(1, glow, ch)
            remote(psp.at[pl.ds(0, 4)], rplace.at[pl.ds(0, 4)], sent.at[9], nbr.at[1], y_up).start()
            remote(psp.at[pl.ds(4, 4)], rplace.at[pl.ds(4, 4)], sent.at[9], nbr.at[1], y_down).start()
        with jax.named_scope("ag1"):
            for ch in range(NCH):
                wait_bytes(NS - 1, agr.at[1, ch], cols(ch))

        with jax.named_scope("proj"):
            for i in range(8):
                rows = pl.ds(i * (data_count // 8), data_count // 8)
                projected = dot_n(glow[...].reshape(PB, D), data_t[:, rows])
                resid[:, rows] = (curv[:, rows] * projected).astype(BF16)

        with jax.named_scope("term"):
            for ch in range(NCH):
                term = dot_n(resid[...], data[:, cols(ch)]) - place[:, cols(ch)]
                if ch == 0:
                    acc[:, cols(ch)] = term
                    wait_bytes(NS, nbr.at[1], slice(None))
                    term = acc[:, cols(ch)]
                term = term - rplace[:, :, cols(ch)].reshape(PB, CW).astype(F32)
                psb[1, :, :, cols(ch)] = term.astype(BF16).reshape(NS, SR, CW)
                rs_send(2, psb.at[1], rbuf.at[1], ch)

        with jax.named_scope("rs2"):
            for ch in range(NCH):
                total = rs_total(2, psb.at[1], rbuf.at[1], ch, NS) + own_force[:, cols(ch)] / prior_var
                out_ref[g, :, cols(ch)] = total.astype(BF16)
                ag_send(2, out_ref, ch)
        with jax.named_scope("ag2"):
            for ch in range(NCH):
                wait_bytes(NS - 1, agr.at[2, ch], cols(ch))

        with jax.named_scope("drain"):
            for k, shares in enumerate((7, 15, 7, 15, 7, 7, 15, 15, 8, 8)):
                ref = rforce.at[pl.ds(0, shares)]
                remote(ref, ref, sent.at[k], nbr.at[0], dev_core).wait_send()

    V = pltpu.VMEM
    S = pltpu.SemaphoreType.DMA
    scratch = [
        V((data_count, D), BF16), V((NS, SR, D), F32), V((1, data_count), jnp.int32),
        V((2 * NS, SR, D), BF16), V((2 * NS, SR, D), BF16), V((PB, data_count), BF16), V((PB, data_count), F32),
        V((2, NS, SR, D), BF16), V((2 * NS, SR, D), BF16), V((NS, SR, D), BF16),
        V((2, NS, SR, D), BF16), V((2 * NS, SR, D), BF16), V((NS, SR, D), BF16), V((NS, SR, D), BF16),
        V((2 * NZ, SR, D), BF16), V((2 * NZ, SR, D), BF16),
        V((2 * PB, NR), F32), V((2 * PB, NR), F32), V((2 * PB, NR), BF16), V((2 * PB, NR), BF16),
        V((PB, D), F32), V((SR, D), F32),
        V((D, data_count), BF16), V((2, PB, DR), F32), V((PB, D), F32), V((2 * PB, D), F32), V((2 * PB, D), F32),
        V((2 * PB, 1), F32),
        S((len(GROUPS) + 2,)), S((10,)), S((3, NCH)), S((3, NCH)), S((3,)), S((3,)), S((2,)),
    ]
    return kernel, scratch


def solution(mesh):
    torus = Mesh(mesh.devices.reshape(2, 4, 8, 2, 2), DP + BLK)

    def shards(particles, data_rows, labels):
        rows, feature_count = particles.shape
        kernel, scratch = make_kernel(feature_count, data_rows.shape[0], rows * 32)
        descent = pl.pallas_call(
            kernel,
            out_shape=jax.ShapeDtypeStruct((8, 16, feature_count), BF16),
            in_specs=[pl.BlockSpec(memory_space=pl.ANY)] * 3,
            out_specs=pl.BlockSpec(memory_space=pltpu.VMEM),
            scratch_shapes=scratch,
            compiler_params=pltpu.CompilerParams(
                collective_id=0, has_side_effects=True, vmem_limit_bytes=44 * 1024 * 1024
            ),
        )(*[pltpu.with_memory_space_constraint(v, pltpu.HBM) for v in (particles.reshape(8, 16, feature_count), data_rows, labels.reshape(1, -1))])
        return descent.reshape(rows, feature_count).astype(F32)

    return jax.shard_map(
        shards,
        mesh=torus,
        in_specs=(P(BLK, None), P(DP, None), P(DP)),
        out_specs=P(BLK, None),
        check_vma=False,
    )
```
